32 devices in a mesh: member: 2 (over x), graph: 8 (over z, y), chan: 2 (over core).
Axes of the slice: x: 2, y: 2, z: 4, core: 2. Of those that a mesh axis runs over, the one named last changes fastest.
Arguments:
- grid_state: bfloat16 [16384, 256], P(('member', 'graph')), parts along dimension 0, may hold values from -6 to 6
- w_src: bfloat16 [256, 512], P(None, 'chan'), may hold values from -0.375 to 0.375
- bias_src: float32 [512], P('chan'), may hold values from -3 to 3
- mesh_embed: bfloat16 [5120, 512], P('graph', 'chan'), may hold values from -6 to 6
- w_node: bfloat16 [512, 512], P('chan'), may hold values from -0.25 to 0.25
- w_dec: bfloat16 [512, 256], P('chan'), may hold values from -0.125 to 0.125
- slot_src: int32 [8, 8, 1024], P('graph'), may hold values from 0 to 1023, as said below
- slot_dst: int32 [8, 8, 1024], P(None, 'graph'), may hold values from 0 to 639, as said below
- slot_count: int32 [8, 8], replicated, may hold values from 1 to 1024, as said below
Outputs:
- grid_out: bfloat16 [16384, 256], P(('member', 'graph'), 'chan'), parts along dimension 0
The draws below stay inside these ranges and needn't reach their ends.
There are 2 independent parts, one for each index of `member`. The reference program is written for one: setup_inputs(seed, part) draws one part's arguments, and reference() takes and returns one part's arrays. A program takes and returns all parts, laid end to end along the dimension named above; an argument that names none is the same for every part. Nothing has to cross between parts.
Inputs may be any that keep to these rules, and one draw needn't show every extreme that they name: `slot_src`: slots at or past the live count hold arbitrary values in the same range. `slot_dst`: slots at or past the live count hold arbitrary values in the same range. slot_count[s, d] counts the live leading slots of the 1024 from shard s to shard d; in every draw some receiving shard has all 1024 slots live from every sender.
All inputs are finite; a program needn't handle non-finite values.
Results may differ from the reference program's by a relative error of at most 0.0056.
Values may be sent and summed in bfloat16 or wider, within the bound.
A program may use at most 64 MiB of HBM per device.

```python
import jax
import jax.numpy as jnp
from jax import lax

C = 256
H = 512
GD = 1024
MD = 640
CAP = 1024
G = 8192
M = 5120
N_GRAPH = 8


def edge_tables(key):
    owners = jnp.arange(N_GRAPH, dtype=jnp.int32)
    offset = jnp.abs(owners[:, None] - owners[None, :])
    cycle_gap = jnp.minimum(offset, N_GRAPH - offset)
    near_bits = jax.random.randint(jax.random.fold_in(key, 12), (N_GRAPH, N_GRAPH), 0, 1 << 20)
    near_count = CAP // 2 + near_bits % (CAP - CAP // 2 + 1)
    levels = jax.random.randint(jax.random.fold_in(key, 11), (N_GRAPH,), 1, 5)
    tail_top = jnp.maximum(levels * (CAP // 16), 1)
    tail_bits = jax.random.randint(jax.random.fold_in(key, 14), (N_GRAPH, N_GRAPH), 0, 1 << 20)
    tail_pick = jax.random.randint(jax.random.fold_in(key, 15), (N_GRAPH, N_GRAPH), 0, 8)
    tail_count = jnp.where(tail_pick == 0, 1 + tail_bits % tail_top[None, :], 1)
    counts = jnp.where(cycle_gap <= 2, near_count, tail_count)
    fullest = jax.random.randint(jax.random.fold_in(key, 13), (), 0, N_GRAPH)
    return jnp.where(owners[None, :] == fullest, CAP, counts).astype(jnp.int32)


def draw_slot_count(key, part):
    return edge_tables(key)


def draw_slot_src(key, part):
    return jax.random.randint(jax.random.fold_in(key, 21), (N_GRAPH, N_GRAPH, CAP), 0, GD).astype(jnp.int32)


def draw_slot_dst(key, part):
    return jax.random.randint(jax.random.fold_in(key, 31), (N_GRAPH, N_GRAPH, CAP), 0, MD).astype(jnp.int32)


def block_scale(own_key, shape, shards, low, high):
    gain = 1.0
    for axis_at, blocks in shards:
        steps = jax.random.uniform(jax.random.fold_in(jax.random.fold_in(own_key, 6), axis_at), (blocks,), jnp.float32, low / len(shards), high / len(shards))
        gain = gain * jnp.repeat(jnp.exp(steps), shape[axis_at] // blocks).reshape((-1,) + (1,) * (len(shape) - 1 - axis_at))
    return gain


def scatter_about(rng, extent, spread, reach, cuts=(), kind=jnp.bfloat16):
    gain = block_scale(rng, extent, cuts, -0.22, 0.18) if cuts else 1.0
    array = jax.random.normal(rng, extent, jnp.float32) * spread * gain
    return jnp.minimum(jnp.maximum(array, -reach), reach).astype(kind)


def setup_inputs(seed: int = 0, part: int = 0) -> dict:
    arg_keys = jax.random.split(jax.random.key(seed), 10)
    own_keys = jax.random.split(jax.random.fold_in(arg_keys[9], part), 10)
    grid_state = scatter_about(own_keys[0], (G, C), 1.0, 6.0, ((0, 8),))
    w_src = scatter_about(arg_keys[1], (C, H), C ** -0.5, 0.375, ((1, 2),))
    bias_src = scatter_about(arg_keys[2], (H,), 0.5, 3.0, ((0, 2),), jnp.float32)
    mesh_embed = scatter_about(arg_keys[3], (M, H), 1.0, 6.0, ((0, 8), (1, 2)))
    w_node = scatter_about(arg_keys[4], (H, H), H ** -0.5, 0.25, ((0, 2),))
    w_dec = scatter_about(arg_keys[5], (H, C), (4 * H) ** -0.5, 0.125, ((0, 2),))
    slot_src = draw_slot_src(jax.random.fold_in(arg_keys[9], 71), part)
    slot_dst = draw_slot_dst(jax.random.fold_in(arg_keys[9], 71), part)
    slot_count = draw_slot_count(jax.random.fold_in(arg_keys[9], 71), part)
    return {"grid_state": grid_state, "w_src": w_src, "bias_src": bias_src, "mesh_embed": mesh_embed, "w_node": w_node, "w_dec": w_dec, "slot_src": slot_src, "slot_dst": slot_dst, "slot_count": slot_count}


def reference(grid_state, w_src, bias_src, mesh_embed, w_node, w_dec, slot_src, slot_dst, slot_count):
    positions = jnp.arange(CAP, dtype=jnp.int32)
    owners = jnp.arange(N_GRAPH, dtype=jnp.int32)

    def send_part(aggregate, sender):
        picked = jnp.take(grid_state, (sender * GD + slot_src[sender]).reshape(-1), axis=0)
        messages = jax.nn.silu(jnp.dot(picked, w_src, preferred_element_type=jnp.float32) + bias_src).astype(jnp.bfloat16)
        usable = (positions[None, :] < slot_count[sender][:, None]).reshape(-1)
        mesh_ids = (owners[:, None] * MD + slot_dst[sender]).reshape(-1).astype(jnp.int32)
        terms = jnp.where(usable[:, None], messages.astype(jnp.float32), jnp.zeros((), jnp.float32))
        return aggregate + jax.ops.segment_sum(terms, mesh_ids, num_segments=N_GRAPH * MD), None

    aggregate, unused = lax.scan(send_part, jnp.zeros((N_GRAPH * MD, H), jnp.float32), owners)
    hidden_pre = jnp.dot(aggregate.astype(jnp.bfloat16), w_node, preferred_element_type=jnp.float32)
    latent = (mesh_embed.astype(jnp.float32) + jax.nn.silu(hidden_pre)).astype(jnp.bfloat16)
    projected = jnp.dot(latent, w_dec, preferred_element_type=jnp.float32).astype(jnp.bfloat16)

    def decode_part(sender):
        usable = (positions[None, :] < slot_count[sender][:, None]).reshape(-1)
        mesh_ids = (owners[:, None] * MD + slot_dst[sender]).reshape(-1).astype(jnp.int32)
        returned = jnp.where(usable[:, None], jnp.take(projected, mesh_ids, axis=0).astype(jnp.float32), jnp.zeros((), jnp.float32))
        decoded = jax.ops.segment_sum(returned, slot_src[sender].reshape(-1).astype(jnp.int32), num_segments=GD)
        own_rows = lax.dynamic_slice_in_dim(grid_state, (sender * GD).astype(jnp.int32), GD, 0)
        return (own_rows.astype(jnp.float32) + decoded).astype(jnp.bfloat16)

    return lax.map(decode_part, owners).reshape(N_GRAPH * GD, C)
```

```python
import functools
import math

import jax
import jax.numpy as jnp
from jax import lax
from jax.experimental import pallas as pl
from jax.experimental.pallas import tpu as pltpu
from jax.sharding import PartitionSpec as P

CHUNKS = 4
SUBS = 2
HOT = jnp.float8_e4m3fn
VMEM_BUDGET = 48 * 2**20
MESH = pl.DeviceIdType.MESH
NT = (((1,), (1,)), ((), ()))


def edge_network(source_rows, w_src, bias_src):
    return jax.nn.silu(
        jnp.dot(source_rows, w_src, preferred_element_type=jnp.float32) + bias_src
    ).astype(jnp.bfloat16)


def segment_rows(values, indices, usable, row_count):
    slot_total = values.shape[0]
    width = values.shape[1]
    block_len = math.gcd(slot_total, 2048)
    block_count = slot_total // block_len
    targets = jnp.where(usable, indices, -1).reshape(block_count, block_len)
    pieces = values.reshape(block_count, block_len, width)
    row_ids = jnp.arange(row_count, dtype=jnp.int32)

    def add_block(summed, scan_item):
        row_target, piece_vals = scan_item
        one_hot = (row_ids[:, None] == row_target[None, :]).astype(jnp.bfloat16)
        return (summed + jnp.dot(one_hot, piece_vals, preferred_element_type=jnp.float32), None)

    result, unused = lax.scan(
        add_block, jnp.zeros((row_count, width), jnp.float32), (targets, pieces)
    )
    return result


def on_device(
    grid_state, w_src, bias_src, mesh_embed, w_node, w_dec, slot_src, slot_dst, slot_count
):
    peers = lax.axis_size("graph")
    own_index = lax.axis_index("graph")
    core_index = lax.axis_index("chan")
    capacity = slot_src.shape[2]
    positions = jnp.arange(capacity, dtype=jnp.int32)
    grid_rows = grid_state.shape[0]
    mesh_rows = mesh_embed.shape[0]
    sent_counts = lax.dynamic_slice_in_dim(slot_count, own_index, 1, 0)[0]
    recv_counts = lax.dynamic_slice_in_dim(slot_count, own_index, 1, 1)[:, 0]
    half_slots = capacity // 2
    chosen = lax.dynamic_slice_in_dim(slot_src[0], core_index * half_slots, half_slots, 1)
    picked = jnp.take(grid_state, chosen.reshape(-1), axis=0).reshape(
        peers, half_slots, grid_state.shape[1]
    )
    arrived = lax.all_to_all(picked, "graph", split_axis=0, concat_axis=0, tiled=True)
    joined = lax.all_gather(arrived, "chan", axis=1, tiled=True)
    messages = edge_network(joined.reshape(peers * capacity, grid_state.shape[1]), w_src, bias_src)
    arrive_ok = (positions[None, :] < recv_counts[:, None]).reshape(-1)
    dst_rows = slot_dst[:, 0, :].reshape(-1)
    aggregate = segment_rows(messages, dst_rows, arrive_ok, mesh_rows)
    partial_hidden = jnp.dot(
        aggregate.astype(jnp.bfloat16), w_node, preferred_element_type=jnp.float32
    )
    hidden_pre = lax.psum_scatter(partial_hidden, "chan", scatter_dimension=1, tiled=True)
    latent = (mesh_embed.astype(jnp.float32) + jax.nn.silu(hidden_pre)).astype(jnp.bfloat16)
    partial_proj = jnp.dot(latent, w_dec, preferred_element_type=jnp.float32)
    projected = lax.psum_scatter(partial_proj, "chan", scatter_dimension=1, tiled=True).astype(
        jnp.bfloat16
    )
    returned = jnp.take(projected, dst_rows, axis=0).reshape(peers, capacity, projected.shape[1])
    came_back = lax.all_to_all(returned, "graph", split_axis=0, concat_axis=0, tiled=True).reshape(
        peers * capacity, projected.shape[1]
    )
    send_ok = (positions[None, :] < sent_counts[:, None]).reshape(-1)
    decoded = segment_rows(came_back, slot_src[0].reshape(-1), send_ok, grid_rows)
    width_half = decoded.shape[1]
    own_cols = lax.dynamic_slice_in_dim(grid_state, core_index * width_half, width_half, 1)
    return (own_cols.astype(jnp.float32) + decoded).astype(jnp.bfloat16)


def silu(v):
    half = 0.5 * v
    return half + half * jnp.tanh(half)


def one_hot(first, rows, indices):
    row_ids = lax.broadcasted_iota(jnp.int32, (rows, indices.shape[1]), 0) + first
    return jnp.where(row_ids == indices, 1.0, 0.0).astype(HOT)


def inner_of(line, lines):
    return line + 1 if line < lines // 2 else line - 1


def outer_of(line, lines):
    return line - 1 if line < lines // 2 else line + 1


def arrival_order(line, lines):
    stages = [(0, 0, line, 1)]
    for source in range(lines):
        gap = abs(source - line)
        if gap:
            stages.append((gap - 1, gap, source, 0))
            stages.append((lines if source == inner_of(line, lines) else gap, gap, source, 1))
    return sorted(stages, key=lambda at: (at[0], at[3], at[1], at[2]))


def link_pieces(line, lines, pieces):
    inner, outer = inner_of(line, lines), outer_of(line, lines)

    def extra(to):
        return pieces if outer_of(to, lines) == line else pieces // 2 if inner_of(to, lines) == line else 0

    up = pieces * (line + 1) + extra(line + 1) if line < lines - 1 else 0
    down = pieces * (lines - line) + extra(line - 1) if line > 0 else 0
    across = pieces * lines - sum(
        pieces if p == outer else pieces - pieces // 2 if p == inner else 0 for p in range(lines) if p != line
    )
    return up, down, across


def graph_kernel(
    peers,
    x_ref, w_src_ref, bias_ref, embed_ref, w_node_ref, w_dec_ref, src_ref, dst_ref, count_ref,
    out_ref,
    x_all, idx_own, idx_in, src_vmem, dst_vmem, count_smem, w_src_all, bias_all, embed_all, w_node_all, w_dec_all,
    enc, dec, hot, msg, agg, acc, proj_mate, proj_all,
    ready, local_sem, par_send, par_recv, idx_send, idx_recv,
    x_send, xz_recv, xy_recv, xm_recv, p_send, pz_recv, py_recv, pm_recv, dec_send, dec_recv,
):
    lines = peers // 2
    me = lax.axis_index("graph")
    core = lax.axis_index("chan")
    mate = 1 - core
    line, side = me // 2, me % 2
    other = line * 2 + (1 - side)
    up, down = (line + 1) * 2 + side, (line - 1) * 2 + side
    has_up, has_down = line < lines - 1, line > 0
    low_half = line < lines // 2
    grid_rows, chans = x_ref.shape
    half_grid = grid_rows // 2
    block = half_grid // CHUNKS
    mesh_rows = embed_ref.shape[0]
    half_mesh = mesh_rows // 2
    part_mesh = half_mesh // SUBS
    cols = chans // 2
    capacity = src_ref.shape[2]
    UP, DOWN, ACROSS, MATE = range(4)

    def remote(src, dst, send, recv, graph, chan):
        return pltpu.make_async_remote_copy(
            src_ref=src, dst_ref=dst, send_sem=send, recv_sem=recv,
            device_id={"graph": graph, "chan": chan}, device_id_type=MESH,
        )

    def by_line(values):
        return sum(jnp.where(line == at, values[at], 0) for at in range(lines))

    inner = jnp.where(low_half, line + 1, line - 1)
    outer = jnp.where(low_half, line - 1, line + 1)
    barrier = pltpu.get_barrier_semaphore()

    def greet(graph, chan):
        pl.semaphore_signal(barrier, inc=1, device_id={"graph": graph, "chan": chan}, device_id_type=MESH)

    greet(me, mate)
    for chan in (core, mate):
        greet(other, chan)
        pl.when(has_up)(functools.partial(greet, up, chan))
        pl.when(has_down)(functools.partial(greet, down, chan))
    my_rows = pl.ds(pl.multiple_of(core * half_mesh, half_mesh), half_mesh)
    mate_rows = pl.ds(pl.multiple_of(mate * half_mesh, half_mesh), half_mesh)
    own_rows = pl.ds(pl.multiple_of(me * grid_rows, grid_rows), grid_rows)
    locals_ = [
        pltpu.make_async_copy(src_ref, src_vmem, local_sem.at[0]),
        pltpu.make_async_copy(dst_ref, dst_vmem, local_sem.at[1]),
        pltpu.make_async_copy(count_ref, count_smem, local_sem.at[2]),
        pltpu.make_async_copy(x_ref, x_all.at[own_rows], local_sem.at[3]),
        pltpu.make_async_copy(w_src_ref, w_src_all.at[core], local_sem.at[4]),
        pltpu.make_async_copy(bias_ref, bias_all.at[core], local_sem.at[5]),
        pltpu.make_async_copy(w_node_ref, w_node_all.at[core], local_sem.at[6]),
        pltpu.make_async_copy(w_dec_ref, w_dec_all.at[core], local_sem.at[7]),
        pltpu.make_async_copy(embed_ref.at[my_rows], embed_all.at[core], local_sem.at[8]),
    ]
    for copy in locals_:
        copy.start()
    for copy in locals_[:3]:
        copy.wait()
    slots = lax.broadcasted_iota(jnp.int32, (1, capacity), 1)
    for to in range(peers):
        idx_own[to, 0:1, :] = jnp.where(slots < count_smem[me, to], src_vmem[0, to : to + 1, :], -1)
        idx_own[to, 1:2, :] = dst_vmem[to]
    idx_in[me] = idx_own[me]
    for copy in locals_[3:]:
        copy.wait()
    pl.semaphore_wait(barrier, 3 + 2 * jnp.where(has_up, 1, 0) + 2 * jnp.where(has_down, 1, 0))

    def send_idx(to):
        remote(idx_own.at[to], idx_in.at[me], idx_send.at[0], idx_recv.at[me], to, core).start()

    def x_part(shard, c, half=core):
        first = shard * grid_rows + c * 2 * block + half * block
        return x_all.at[pl.ds(pl.multiple_of(first, block), block)]

    send_idx(other)
    pl.when(has_up)(functools.partial(send_idx, up))
    pl.when(has_down)(functools.partial(send_idx, down))
    for c in range(CHUNKS):
        ref = x_part(me, c)
        for at, going, to, recv in (
            (UP, has_up, up, xz_recv), (DOWN, has_down, down, xz_recv), (ACROSS, None, other, xy_recv),
        ):
            def go(ref=ref, at=at, to=to, recv=recv, c=c):
                remote(ref, ref, x_send.at[at], recv.at[line, c], to, core).start()
            if going is None:
                go()
            else:
                pl.when(going)(go)
    par_copies = [
        remote(w_src_all.at[core], w_src_all.at[core], par_send.at[0], par_recv.at[0], me, mate),
        remote(bias_all.at[core], bias_all.at[core], par_send.at[1], par_recv.at[1], me, mate),
        remote(embed_ref.at[mate_rows], embed_all.at[core], par_send.at[2], par_recv.at[2], me, mate),
        remote(w_node_all.at[core], w_node_all.at[core], par_send.at[3], par_recv.at[3], me, mate),
        remote(w_dec_all.at[core], w_dec_all.at[core], par_send.at[4], par_recv.at[4], me, mate),
    ]
    for copy in par_copies:
        copy.start()

    def tell(at, to):
        pl.semaphore_signal(ready.at[at], inc=1, device_id={"graph": to, "chan": core}, device_id_type=MESH)

    pl.when(line == 0)(functools.partial(tell, 0, up))
    pl.when(line == lines - 1)(functools.partial(tell, 1, down))

    def relays(part, send, z_recv, y_recv, late, arrived):
        def extra(q, to):
            shard = line * 2 + 1 - side
            ref = part(shard, q)
            remote(ref, ref, send.at[UP if to == "up" else DOWN], y_recv.at[line, q],
                   up if to == "up" else down, core).start()

        def extra_going(to, q):
            going, at, target_low = (
                (has_up, line + 1, line + 1 < lines // 2) if to == "up" else (has_down, line - 1, line - 1 < lines // 2)
            )
            full = target_low if to == "up" else jnp.logical_not(target_low)
            return going if late(q) else going & full

        def last_stage(to):
            return line - 1 if to == "up" else lines - 2 - line

        def extras(i, q):
            for to in ("up", "down"):
                pl.when(extra_going(to, q) & (last_stage(to) == i))(functools.partial(extra, q, to))

        def take_line(i, q, which):
            for above in (True, False):
                source = line + 1 + i if above else line - 1 - i
                valid = (source < lines) if above else (source >= 0)
                if which is not None:
                    valid = valid & ((low_half if above else jnp.logical_not(low_half)) == (which == "inner"))
                onward, to, at = (has_down, down, DOWN) if above else (has_up, up, UP)

                @pl.when(valid)
                def _(source=source, onward=onward, to=to, at=at):
                    ref = part(source * 2 + side, q)
                    remote(ref, ref, send.at[at], z_recv.at[source, q], me, mate).wait_recv()

                    @pl.when(onward)
                    def _():
                        remote(ref, ref, send.at[at], z_recv.at[source, q], to, core).start()

                    crossing = source != outer
                    if late(q):
                        crossing = crossing & (source != inner)

                    @pl.when(crossing)
                    def _():
                        remote(ref, ref, send.at[ACROSS], y_recv.at[source, q], other, core).start()

                    arrived(source * 2 + side, q)

        def take_other(i, q):
            def take(source):
                shard = source * 2 + 1 - side
                ref = part(shard, q)
                remote(ref, ref, send.at[ACROSS], y_recv.at[source, q], me, mate).wait_recv()
                arrived(shard, q)

            if i == 0:
                take(line)
                extras(-1, q)
                return
            for source, valid in ((line + i, line + i < lines), (line - i, line - i >= 0)):
                if late(q):
                    valid = valid & (source != inner)
                pl.when(valid)(functools.partial(take, source))

        def take_inner(q):
            shard = inner * 2 + 1 - side
            ref = part(shard, q)
            remote(ref, ref, send.at[ACROSS], y_recv.at[inner, q], me, mate).wait_recv()
            arrived(shard, q)

        return take_line, take_other, take_inner, extras

    def to_mate(shard, c):
        ref = x_part(shard, c)
        remote(ref, ref, x_send.at[MATE], xm_recv.at[shard], me, mate).start()

    nearest = [sorted((p for p in range(lines) if p != at), key=lambda p: (abs(p - at), p)) for at in range(lines)]
    build_order = [me, other]
    for i in range(lines - 1):
        source = by_line([nearest[at][i] for at in range(lines)])
        build_order += [source * 2 + side, source * 2 + 1 - side]
    tables = [arrival_order(at, lines) for at in range(lines)]
    order = []
    for k in range(peers - 1):
        source = by_line([tables[at][k][2] for at in range(lines)])
        flip = by_line([tables[at][k][3] for at in range(lines)])
        stage = max(tables[at][k][0] for at in range(lines))
        order.append((stage, source * 2 + jnp.where(flip == 1, 1 - side, side)))

    def build_enc(shard, wait=True):
        if wait:
            remote(idx_own.at[0], idx_in.at[shard], idx_send.at[0], idx_recv.at[shard], me, mate).wait_recv()
        hot[:half_mesh, :] = one_hot(core * half_mesh, half_mesh, dst_vmem[shard])
        for t in range(2):
            picks = one_hot(t * half_grid, half_grid, idx_in[shard, 0:1, :])
            enc[shard, :, t * half_grid : (t + 1) * half_grid] = lax.dot_general(
                hot[:half_mesh, :], picks, NT, preferred_element_type=jnp.float32
            ).astype(jnp.bfloat16)

    pending = []

    def dec_copy(shard, half):
        ref = dec.at[shard, pl.ds(pl.multiple_of(half * half_grid, half_grid), half_grid)]
        return remote(ref, ref, dec_send.at[0], dec_recv.at[shard], me, mate)

    def flush():
        while pending:
            dec_copy(pending.pop(0), core).start()

    def build_dec(shard):
        flush()
        hot[...] = one_hot(0, mesh_rows, idx_in[shard, 1:2, :])
        for t in range(half_grid // 256):
            first = pl.multiple_of(core * half_grid, half_grid) + t * 256
            picks = one_hot(first, 256, idx_own[shard, 0:1, :])
            dec[shard, pl.ds(pl.multiple_of(first, 256), 256), :] = lax.dot_general(
                picks, hot[...], NT, preferred_element_type=jnp.float32
            ).astype(jnp.bfloat16)
        pending.append(shard)

    def encode(shard, first=False):
        if not first:
            whole = x_all.at[pl.ds(0, half_grid)]
            remote(whole, whole, x_send.at[MATE], xm_recv.at[shard], me, mate).wait_recv()
        for c in range(CHUNKS):
            rows = pl.ds(pl.multiple_of(shard * grid_rows, grid_rows) + c * 2 * block, 2 * block)
            for h in range(2):
                pre = jnp.dot(x_all[rows, :], w_src_all[h], preferred_element_type=jnp.float32) + bias_all[h]
                msg[c * 2 * block : (c + 1) * 2 * block, h * (msg.shape[1] // 2) : (h + 1) * (msg.shape[1] // 2)] = (
                    pre + pre * jnp.tanh(pre)
                ).astype(jnp.bfloat16)
        total = jnp.dot(enc[shard], msg[...], preferred_element_type=jnp.float32)
        if first:
            agg[...] = total
        else:
            agg[...] += total

    build_enc(me, wait=False)
    for copy in par_copies:
        copy.wait()
    w_src_all[...] = w_src_all[...] * 0.5
    bias_all[...] = bias_all[...] * 0.5
    encode(me, first=True)

    @pl.when(has_down)
    def _():
        pl.semaphore_wait(ready.at[0], 1)
        pl.when(has_up)(functools.partial(tell, 0, up))

    @pl.when(has_up)
    def _():
        pl.semaphore_wait(ready.at[1], 1)
        pl.when(has_down)(functools.partial(tell, 1, down))

    for source in range(lines):
        for its_side in range(2):
            to = source * 2 + its_side
            same = side == its_side
            near = jnp.where(same, jnp.abs(line - source) <= 1, line == source)
            pl.when(jnp.logical_not(near))(functools.partial(send_idx, to))

    tasks = [functools.partial(build_enc, shard) for shard in build_order[1:]]
    dec_tasks = [functools.partial(build_dec, shard) for shard in build_order]

    def run(count):
        for _ in range(count):
            if tasks:
                tasks.pop(0)()
            elif dec_tasks:
                dec_tasks.pop(0)()

    def halves(c):
        return c >= CHUNKS // 2

    take_line, take_other, take_inner, extras = relays(x_part, x_send, xz_recv, xy_recv, halves, to_mate)
    for i in range(lines):
        for c in range(CHUNKS):
            if i < lines - 1:
                take_line(i, c, None)
            take_other(i, c)
            if i < lines - 1:
                run(-(-len(tasks) // (CHUNKS - c)) if i else 1)
            elif tasks:
                run(1)
        for c in range(CHUNKS):
            extras(i, c)
        tasks.extend(functools.partial(encode, shard) for stage, shard in order if stage == i)
    for c in range(CHUNKS // 2, CHUNKS):
        take_inner(c)
    tasks.extend(functools.partial(encode, shard) for stage, shard in order if stage == lines)
    while tasks:
        tasks.pop(0)()

    hidden_cols = agg.shape[1]
    width = hidden_cols // 2
    hidden = sum(
        jnp.dot(agg[:, h * width : (h + 1) * width].astype(jnp.bfloat16), w_node_all[h], preferred_element_type=jnp.float32)
        for h in range(2)
    )
    projected = sum(
        jnp.dot(
            (
                embed_all[h].astype(jnp.float32) + silu(hidden[:, h * width : (h + 1) * width])
            ).astype(jnp.bfloat16),
            w_dec_all[h], preferred_element_type=jnp.float32,
        )
        for h in range(2)
    ).astype(jnp.bfloat16)
    my_first = pl.multiple_of(me * mesh_rows + core * half_mesh, half_mesh)

    @pl.when(core == 0)
    def _():
        proj_all[pl.ds(my_first, half_mesh), :] = projected[:, :cols]
        proj_mate[...] = projected[:, cols:]

    @pl.when(core == 1)
    def _():
        proj_all[pl.ds(my_first, half_mesh), :] = projected[:, cols:]
        proj_mate[...] = projected[:, :cols]

    def p_part(shard, q):
        flip, sub = q % 2, q // 2
        half = mate if flip else core
        first = shard * mesh_rows + half * half_mesh + sub * part_mesh
        return proj_all.at[pl.ds(pl.multiple_of(first, part_mesh), part_mesh)]

    for sub in range(SUBS):
        into = p_part(me, 2 * sub)
        for flip in range(2):
            ref = proj_mate.at[pl.ds(sub * part_mesh, part_mesh)] if flip else into
            chan = mate if flip else core
            for at, going, to, recv in (
                (UP, has_up, up, pz_recv), (DOWN, has_down, down, pz_recv), (ACROSS, None, other, py_recv),
            ):
                def go(ref=ref, into=into, at=at, to=to, recv=recv, q=2 * sub + flip, chan=chan):
                    remote(ref, into, p_send.at[at], recv.at[line, q], to, chan).start()
                if going is None:
                    go()
                else:
                    pl.when(going)(go)
    whole_half = proj_all.at[pl.ds(my_first, half_mesh)]
    remote(proj_mate, whole_half, p_send.at[MATE], pm_recv.at[0], me, mate).start()

    def decode(shard, first=False):
        remote(dec.at[0, pl.ds(0, half_grid)], dec.at[0, pl.ds(0, half_grid)], dec_send.at[0], dec_recv.at[shard], me, mate).wait_recv()
        rows = pl.ds(pl.multiple_of(shard * mesh_rows, mesh_rows), mesh_rows)
        for t in range(2):
            at = pl.ds(t * half_grid, half_grid)
            acc[at, :] += jnp.dot(dec[shard, at, :], proj_all[rows, :], preferred_element_type=jnp.float32)

    tasks = dec_tasks[:]
    take_line, take_other, take_inner, extras = relays(
        p_part, p_send, pz_recv, py_recv, lambda q: q >= SUBS, lambda shard, q: None)
    acc[...] = x_all[own_rows, pl.ds(pl.multiple_of(core * cols, cols), cols)].astype(jnp.float32)

    def own_decode():
        remote(proj_mate, whole_half, p_send.at[MATE], pm_recv.at[0], me, mate).wait_recv()
        decode(me)

    tasks.append(flush)
    tasks.append(own_decode)
    late_tasks = []
    for _ in range(2):
        tasks.pop(0)()
    pieces = 2 * SUBS
    for i in range(lines):
        if i < lines - 1:
            for q in range(pieces):
                take_line(i, q, "inner")
                if tasks and q % 2:
                    tasks.pop(0)()
        for q in range(pieces):
            take_other(i, q)
            if i < lines - 1:
                take_line(i, q, "outer")
            if tasks:
                tasks.pop(0)()
        for q in range(pieces):
            extras(i, q)
        tasks.extend(functools.partial(decode, shard) for stage, shard in order if stage == i)
    for q in range(SUBS, pieces):
        take_inner(q)
    tasks.extend(functools.partial(decode, shard) for stage, shard in order if stage == lines)
    while tasks:
        tasks.pop(0)()
    out_ref[...] = acc[...].astype(jnp.bfloat16)

    def drained(ref, sem):
        remote(ref, ref, sem, sem, me, mate).wait_send()

    for at in range(lines):
        @pl.when(line == at)
        def _(at=at):
            for n, (x_n, p_n) in enumerate(zip(link_pieces(at, lines, CHUNKS), link_pieces(at, lines, pieces))):
                if x_n:
                    drained(x_all.at[pl.ds(0, x_n * block)], x_send.at[n])
                    drained(proj_all.at[pl.ds(0, p_n * part_mesh)], p_send.at[n])
    drained(x_all.at[pl.ds(0, (peers - 1) * half_grid)], x_send.at[MATE])
    drained(proj_mate, p_send.at[MATE])
    drained(idx_own.at[pl.ds(0, peers - 1)], idx_send.at[0])
    drained(dec.at[:, pl.ds(0, half_grid)], dec_send.at[0])


def fused(grid_state, w_src, bias_src, mesh_embed, w_node, w_dec, slot_src, slot_dst, slot_count):
    peers = lax.axis_size("graph")
    capacity = slot_src.shape[2]
    grid_rows, chans = grid_state.shape
    mesh_rows = mesh_embed.shape[0]
    hidden = w_src.shape[1]
    lines = peers // 2
    bf16, f32, i32 = jnp.bfloat16, jnp.float32, jnp.int32
    dma = pltpu.SemaphoreType.DMA
    pieces = 2 * SUBS
    return pl.pallas_call(
        functools.partial(graph_kernel, peers),
        out_shape=jax.ShapeDtypeStruct((grid_rows, chans // 2), bf16),
        in_specs=[pl.BlockSpec(memory_space=pl.ANY)] * 9,
        out_specs=pl.BlockSpec(memory_space=pltpu.VMEM),
        scratch_shapes=[
            pltpu.VMEM((peers * grid_rows, chans), bf16),
            pltpu.VMEM((peers, 2, capacity), i32),
            pltpu.VMEM((peers, 2, capacity), i32),
            pltpu.VMEM(slot_src.shape, i32),
            pltpu.VMEM(slot_dst.shape, i32),
            pltpu.SMEM(slot_count.shape, i32),
            pltpu.VMEM((2,) + w_src.shape, bf16),
            pltpu.VMEM((2, 1, hidden), f32),
            pltpu.VMEM((2, mesh_rows // 2, hidden), bf16),
            pltpu.VMEM((2,) + w_node.shape, bf16),
            pltpu.VMEM((2,) + w_dec.shape, bf16),
            pltpu.VMEM((peers, mesh_rows // 2, grid_rows), bf16),
            pltpu.VMEM((peers, grid_rows, mesh_rows), bf16),
            pltpu.VMEM((mesh_rows, capacity), HOT),
            pltpu.VMEM((grid_rows, 2 * hidden), bf16),
            pltpu.VMEM((mesh_rows // 2, 2 * hidden), f32),
            pltpu.VMEM((grid_rows, chans // 2), f32),
            pltpu.VMEM((mesh_rows // 2, chans // 2), bf16),
            pltpu.VMEM((peers * mesh_rows, chans // 2), bf16),
            pltpu.SemaphoreType.REGULAR((2,)),
            dma((9,)), dma((5,)), dma((5,)), dma((1,)), dma((peers,)),
            dma((4,)), dma((lines, CHUNKS)), dma((lines, CHUNKS)), dma((peers,)),
            dma((4,)), dma((lines, pieces)), dma((lines, pieces)), dma((1,)), dma((1,)), dma((peers,)),
        ],
        compiler_params=pltpu.CompilerParams(collective_id=0, has_side_effects=True),
    )(grid_state, w_src, bias_src[None, :], mesh_embed, w_node, w_dec, slot_src, slot_dst, slot_count)


def held_bytes(peers, grid_state, mesh_embed, *rest):
    grid_rows, chans = grid_state.shape
    mesh_rows = mesh_embed.shape[0]
    return 2 * peers * grid_rows * (chans + 2 * mesh_rows)


def per_device(grid_state, w_src, bias_src, mesh_embed, *rest):
    peers = lax.axis_size("graph")
    fits = (
        peers % 2 == 0
        and peers >= 4
        and lax.axis_size("chan") == 2
        and held_bytes(peers, grid_state, mesh_embed) <= VMEM_BUDGET
    )
    body = fused if fits else on_device
    return body(grid_state, w_src, bias_src, mesh_embed, *rest)


def solution(mesh):
    placed = (
        P(("member", "graph"), None),
        P(None, "chan"),
        P("chan"),
        P("graph", "chan"),
        P("chan", None),
        P("chan", None),
        P("graph", None, None),
        P(None, "graph", None),
        P(),
    )
    return jax.shard_map(
        per_device,
        mesh=mesh,
        in_specs=placed,
        out_specs=P(("member", "graph"), "chan"),
        check_vma=False,
    )
```

```python
import functools
import math

import jax
import jax.numpy as jnp
from jax import lax
from jax.experimental import pallas as pl
from jax.experimental.pallas import tpu as pltpu
from jax.sharding import PartitionSpec as P

CHUNKS = 4
SUBS = 2
HOT = jnp.float8_e4m3fn
VMEM_BUDGET = 48 * 2**20
MESH = pl.DeviceIdType.MESH
NT = (((1,), (1,)), ((), ()))


def edge_network(source_rows, w_src, bias_src):
    return jax.nn.silu(
        jnp.dot(source_rows, w_src, preferred_element_type=jnp.float32) + bias_src
    ).astype(jnp.bfloat16)


def segment_rows(values, indices, usable, row_count):
    slot_total = values.shape[0]
    width = values.shape[1]
    block_len = math.gcd(slot_total, 2048)
    block_count = slot_total // block_len
    targets = jnp.where(usable, indices, -1).reshape(block_count, block_len)
    pieces = values.reshape(block_count, block_len, width)
    row_ids = jnp.arange(row_count, dtype=jnp.int32)

    def add_block(summed, scan_item):
        row_target, piece_vals = scan_item
        one_hot = (row_ids[:, None] == row_target[None, :]).astype(jnp.bfloat16)
        return (summed + jnp.dot(one_hot, piece_vals, preferred_element_type=jnp.float32), None)

    result, unused = lax.scan(
        add_block, jnp.zeros((row_count, width), jnp.float32), (targets, pieces)
    )
    return result


def on_device(
    grid_state, w_src, bias_src, mesh_embed, w_node, w_dec, slot_src, slot_dst, slot_count
):
    peers = lax.axis_size("graph")
    own_index = lax.axis_index("graph")
    core_index = lax.axis_index("chan")
    capacity = slot_src.shape[2]
    positions = jnp.arange(capacity, dtype=jnp.int32)
    grid_rows = grid_state.shape[0]
    mesh_rows = mesh_embed.shape[0]
    sent_counts = lax.dynamic_slice_in_dim(slot_count, own_index, 1, 0)[0]
    recv_counts = lax.dynamic_slice_in_dim(slot_count, own_index, 1, 1)[:, 0]
    half_slots = capacity // 2
    chosen = lax.dynamic_slice_in_dim(slot_src[0], core_index * half_slots, half_slots, 1)
    picked = jnp.take(grid_state, chosen.reshape(-1), axis=0).reshape(
        peers, half_slots, grid_state.shape[1]
    )
    arrived = lax.all_to_all(picked, "graph", split_axis=0, concat_axis=0, tiled=True)
    joined = lax.all_gather(arrived, "chan", axis=1, tiled=True)
    messages = edge_network(joined.reshape(peers * capacity, grid_state.shape[1]), w_src, bias_src)
    arrive_ok = (positions[None, :] < recv_counts[:, None]).reshape(-1)
    dst_rows = slot_dst[:, 0, :].reshape(-1)
    aggregate = segment_rows(messages, dst_rows, arrive_ok, mesh_rows)
    partial_hidden = jnp.dot(
        aggregate.astype(jnp.bfloat16), w_node, preferred_element_type=jnp.float32
    )
    hidden_pre = lax.psum_scatter(partial_hidden, "chan", scatter_dimension=1, tiled=True)
    latent = (mesh_embed.astype(jnp.float32) + jax.nn.silu(hidden_pre)).astype(jnp.bfloat16)
    partial_proj = jnp.dot(latent, w_dec, preferred_element_type=jnp.float32)
    projected = lax.psum_scatter(partial_proj, "chan", scatter_dimension=1, tiled=True).astype(
        jnp.bfloat16
    )
    returned = jnp.take(projected, dst_rows, axis=0).reshape(peers, capacity, projected.shape[1])
    came_back = lax.all_to_all(returned, "graph", split_axis=0, concat_axis=0, tiled=True).reshape(
        peers * capacity, projected.shape[1]
    )
    send_ok = (positions[None, :] < sent_counts[:, None]).reshape(-1)
    decoded = segment_rows(came_back, slot_src[0].reshape(-1), send_ok, grid_rows)
    width_half = decoded.shape[1]
    own_cols = lax.dynamic_slice_in_dim(grid_state, core_index * width_half, width_half, 1)
    return (own_cols.astype(jnp.float32) + decoded).astype(jnp.bfloat16)


def silu(v):
    half = 0.5 * v
    return half + half * jnp.tanh(half)


def one_hot(first, rows, indices):
    row_ids = lax.broadcasted_iota(jnp.int32, (rows, indices.shape[1]), 0) + first
    return jnp.where(row_ids == indices, 1.0, 0.0).astype(HOT)


def far_of(line, lines):
    return lines - 1 if line < lines // 2 else 0


def is_end(line, lines):
    return line in (0, lines - 1)


def given(line, lines):
    outer = line - 1 if line < lines // 2 else line + 1
    return outer if not is_end(line, lines) and is_end(outer, lines) else None


def arrival_order(line, lines):
    stages = [(0, 1, 0, line)]
    for source in range(lines):
        gap = abs(source - line)
        if gap:
            split = is_end(line, lines) and source == far_of(line, lines)
            stages += [(gap - 1, 0, gap, source), (lines if split else gap, 1, gap, source)]
    return sorted(stages)


def link_pieces(line, lines, pieces):
    def extra(to):
        if not 0 <= to < lines:
            return 0
        return pieces // 2 if is_end(to, lines) else pieces if given(to, lines) == line else 0

    up = pieces * (line + 1) + extra(line + 1) if line < lines - 1 else 0
    down = pieces * (lines - line) + extra(line - 1) if line > 0 else 0
    across = pieces * lines
    if given(line, lines) is not None:
        across -= pieces
    if is_end(line, lines):
        across -= pieces // 2
    return up, down, across


def graph_kernel(
    peers,
    x_ref, w_src_ref, bias_ref, embed_ref, w_node_ref, w_dec_ref, src_ref, dst_ref, count_ref,
    out_ref,
    x_all, idx_own, idx_in, src_vmem, dst_vmem, count_smem, w_src_all, bias_all, embed_all, w_node_all, w_dec_all,
    enc, dec, hot, msg, agg, acc, proj_mate, proj_all,
    ready, local_sem, par_send, par_recv, idx_send, idx_recv,
    x_send, xz_recv, xy_recv, xm_recv, p_send, pz_recv, py_recv, pm_recv, dec_send, dec_recv,
):
    lines = peers // 2
    me = lax.axis_index("graph")
    core = lax.axis_index("chan")
    mate = 1 - core
    line, side = me // 2, me % 2
    other = line * 2 + (1 - side)
    up, down = (line + 1) * 2 + side, (line - 1) * 2 + side
    has_up, has_down = line < lines - 1, line > 0
    low_half = line < lines // 2
    grid_rows, chans = x_ref.shape
    half_grid = grid_rows // 2
    block = half_grid // CHUNKS
    mesh_rows = embed_ref.shape[0]
    half_mesh = mesh_rows // 2
    part_mesh = half_mesh // SUBS
    cols = chans // 2
    capacity = src_ref.shape[2]
    UP, DOWN, ACROSS, MATE = range(4)

    def remote(src, dst, send, recv, graph, chan):
        return pltpu.make_async_remote_copy(
            src_ref=src, dst_ref=dst, send_sem=send, recv_sem=recv,
            device_id={"graph": graph, "chan": chan}, device_id_type=MESH,
        )

    def by_line(values):
        return sum(jnp.where(line == at, values[at], 0) for at in range(lines))

    end = (line == 0) | (line == lines - 1)
    far = jnp.where(low_half, lines - 1, 0)
    giver = by_line([-1 if given(at, lines) is None else given(at, lines) for at in range(lines)])
    barrier = pltpu.get_barrier_semaphore()

    def greet(graph, chan):
        pl.semaphore_signal(barrier, inc=1, device_id={"graph": graph, "chan": chan}, device_id_type=MESH)

    greet(me, mate)
    for chan in (core, mate):
        greet(other, chan)
        pl.when(has_up)(functools.partial(greet, up, chan))
        pl.when(has_down)(functools.partial(greet, down, chan))
    my_rows = pl.ds(pl.multiple_of(core * half_mesh, half_mesh), half_mesh)
    mate_rows = pl.ds(pl.multiple_of(mate * half_mesh, half_mesh), half_mesh)
    own_rows = pl.ds(pl.multiple_of(me * grid_rows, grid_rows), grid_rows)
    locals_ = [
        pltpu.make_async_copy(src_ref, src_vmem, local_sem.at[0]),
        pltpu.make_async_copy(dst_ref, dst_vmem, local_sem.at[1]),
        pltpu.make_async_copy(count_ref, count_smem, local_sem.at[2]),
        pltpu.make_async_copy(x_ref, x_all.at[own_rows], local_sem.at[3]),
        pltpu.make_async_copy(w_src_ref, w_src_all.at[core], local_sem.at[4]),
        pltpu.make_async_copy(bias_ref, bias_all.at[core], local_sem.at[5]),
        pltpu.make_async_copy(w_node_ref, w_node_all.at[core], local_sem.at[6]),
        pltpu.make_async_copy(w_dec_ref, w_dec_all.at[core], local_sem.at[7]),
        pltpu.make_async_copy(embed_ref.at[my_rows], embed_all.at[core], local_sem.at[8]),
    ]
    for copy in locals_:
        copy.start()
    for copy in locals_[:3]:
        copy.wait()
    slots = lax.broadcasted_iota(jnp.int32, (1, capacity), 1)
    for to in range(peers):
        idx_own[to, 0:1, :] = jnp.where(slots < count_smem[me, to], src_vmem[0, to : to + 1, :], -1)
        idx_own[to, 1:2, :] = dst_vmem[to]
    idx_in[me] = idx_own[me]
    for copy in locals_[3:]:
        copy.wait()
    pl.semaphore_wait(barrier, 3 + 2 * jnp.where(has_up, 1, 0) + 2 * jnp.where(has_down, 1, 0))

    def send_idx(to):
        remote(idx_own.at[to], idx_in.at[me], idx_send.at[0], idx_recv.at[me], to, core).start()

    def x_part(shard, c, half=core):
        first = shard * grid_rows + c * 2 * block + half * block
        return x_all.at[pl.ds(pl.multiple_of(first, block), block)]

    send_idx(other)
    pl.when(has_up)(functools.partial(send_idx, up))
    pl.when(has_down)(functools.partial(send_idx, down))

    def send_own(c):
        ref = x_part(me, c)
        for at, going, to, recv in (
            (UP, has_up, up, xz_recv), (DOWN, has_down, down, xz_recv), (ACROSS, None, other, xy_recv),
        ):
            def go(at=at, to=to, recv=recv):
                remote(ref, ref, x_send.at[at], recv.at[line, c], to, core).start()
            if going is None:
                go()
            else:
                pl.when(going)(go)

    for c in range(CHUNKS // 2):
        send_own(c)
    par_copies = [
        remote(w_src_all.at[core], w_src_all.at[core], par_send.at[0], par_recv.at[0], me, mate),
        remote(bias_all.at[core], bias_all.at[core], par_send.at[1], par_recv.at[1], me, mate),
        remote(embed_ref.at[mate_rows], embed_all.at[core], par_send.at[2], par_recv.at[2], me, mate),
        remote(w_node_all.at[core], w_node_all.at[core], par_send.at[3], par_recv.at[3], me, mate),
        remote(w_dec_all.at[core], w_dec_all.at[core], par_send.at[4], par_recv.at[4], me, mate),
    ]
    for copy in par_copies:
        copy.start()

    def tell(at, to):
        pl.semaphore_signal(ready.at[at], inc=1, device_id={"graph": to, "chan": core}, device_id_type=MESH)

    pl.when(line == 0)(functools.partial(tell, 0, up))
    pl.when(line == lines - 1)(functools.partial(tell, 1, down))

    def relays(part, send, z_recv, y_recv, late, arrived):
        def extra(source, q, above):
            ref = part(source * 2 + 1 - side, q)
            remote(ref, ref, send.at[UP if above else DOWN], y_recv.at[source, q], up if above else down, core).start()

        def extras(source, q):
            for above, there in ((True, has_up), (False, has_down)):
                to = line + 1 if above else line - 1
                to_end = (to == 0) | (to == lines - 1)
                to_giver = by_line([
                    -1 if not 0 <= at + (1 if above else -1) < lines
                    or given(at + (1 if above else -1), lines) is None
                    else given(at + (1 if above else -1), lines)
                    for at in range(lines)
                ])
                wanted = (source == line) & (to_giver == line)
                if late(q):
                    wanted = wanted | (to_end & (source == jnp.where(to < lines // 2, lines - 1, 0)))
                pl.when(there & wanted)(functools.partial(extra, source, q, above))

        def take_line(i, q, which):
            for above in (True, False):
                source = line + 1 + i if above else line - 1 - i
                valid = (source < lines) if above else (source >= 0)
                if which is not None:
                    valid = valid & ((low_half if above else jnp.logical_not(low_half)) == (which == "inner"))
                onward, to, at = (has_down, down, DOWN) if above else (has_up, up, UP)

                @pl.when(valid)
                def _(source=source, onward=onward, to=to, at=at):
                    ref = part(source * 2 + side, q)
                    remote(ref, ref, send.at[at], z_recv.at[source, q], me, mate).wait_recv()

                    @pl.when(onward)
                    def _():
                        remote(ref, ref, send.at[at], z_recv.at[source, q], to, core).start()

                    crossing = source != giver
                    if late(q):
                        crossing = crossing & jnp.logical_not(end & (source == far))

                    @pl.when(crossing)
                    def _():
                        remote(ref, ref, send.at[ACROSS], y_recv.at[source, q], other, core).start()

                    arrived(source * 2 + side, q)

        def take_other(i, q):
            def take(source):
                shard = source * 2 + 1 - side
                ref = part(shard, q)
                remote(ref, ref, send.at[ACROSS], y_recv.at[source, q], me, mate).wait_recv()
                extras(source, q)
                arrived(shard, q)

            if i == 0:
                take(line)
                return
            for source, valid in ((line + i, line + i < lines), (line - i, line - i >= 0)):
                if late(q):
                    valid = valid & jnp.logical_not(end & (source == far))
                pl.when(valid)(functools.partial(take, source))

        def take_far(q):
            pl.when(end)(functools.partial(take_one, far, q))

        def take_one(source, q):
            shard = source * 2 + 1 - side
            ref = part(shard, q)
            remote(ref, ref, send.at[ACROSS], y_recv.at[source, q], me, mate).wait_recv()
            arrived(shard, q)

        return take_line, take_other, take_far

    def to_mate(shard, c):
        ref = x_part(shard, c)
        remote(ref, ref, x_send.at[MATE], xm_recv.at[shard, c // (CHUNKS // 2)], me, mate).start()

    nearest = [sorted((p for p in range(lines) if p != at), key=lambda p: (abs(p - at), p)) for at in range(lines)]
    build_order = [me, other]
    for i in range(lines - 1):
        source = by_line([nearest[at][i] for at in range(lines)])
        build_order += [source * 2 + side, source * 2 + 1 - side]
    tables = [arrival_order(at, lines) for at in range(lines)]
    order = []
    for k in range(peers - 1):
        source = by_line([tables[at][k][3] for at in range(lines)])
        flip = by_line([tables[at][k][1] for at in range(lines)])
        stage = max(tables[at][k][0] for at in range(lines))
        order.append((stage, source * 2 + jnp.where(flip == 1, 1 - side, side)))

    def build_enc(shard, wait=True):
        if wait:
            remote(idx_own.at[0], idx_in.at[shard], idx_send.at[0], idx_recv.at[shard], me, mate).wait_recv()
        hot[:half_mesh, :] = one_hot(core * half_mesh, half_mesh, dst_vmem[shard])
        for t in range(2):
            picks = one_hot(t * half_grid, half_grid, idx_in[shard, 0:1, :])
            enc[shard, :, t * half_grid : (t + 1) * half_grid] = lax.dot_general(
                hot[:half_mesh, :], picks, NT, preferred_element_type=jnp.float32
            ).astype(jnp.bfloat16)

    pending = []

    def dec_copy(shard, half):
        ref = dec.at[shard, pl.ds(pl.multiple_of(half * half_grid, half_grid), half_grid)]
        return remote(ref, ref, dec_send.at[0], dec_recv.at[shard], me, mate)

    def flush():
        while pending:
            dec_copy(pending.pop(0), core).start()

    def build_dec(shard, wait=True):
        flush()
        hot[...] = one_hot(0, mesh_rows, idx_in[shard, 1:2, :])
        for t in range(half_grid // 256):
            first = pl.multiple_of(core * half_grid, half_grid) + t * 256
            picks = one_hot(first, 256, idx_own[shard, 0:1, :])
            dec[shard, pl.ds(pl.multiple_of(first, 256), 256), :] = lax.dot_general(
                picks, hot[...], NT, preferred_element_type=jnp.float32
            ).astype(jnp.bfloat16)
        pending.append(shard)

    def encode(shard, first=False, parts=(0, 1)):
        if not first:
            for part in parts:
                some = x_all.at[pl.ds(0, half_grid // 2)]
                remote(some, some, x_send.at[MATE], xm_recv.at[shard, part], me, mate).wait_recv()
        low, high = min(parts) * CHUNKS // 2, (max(parts) + 1) * CHUNKS // 2
        for c in range(low, high):
            rows = pl.ds(pl.multiple_of(shard * grid_rows, grid_rows) + c * 2 * block, 2 * block)
            for h in range(2):
                pre = jnp.dot(x_all[rows, :], w_src_all[h], preferred_element_type=jnp.float32) + bias_all[h]
                msg[c * 2 * block : (c + 1) * 2 * block, h * (msg.shape[1] // 2) : (h + 1) * (msg.shape[1] // 2)] = (
                    pre + pre * jnp.tanh(pre)
                ).astype(jnp.bfloat16)
        some = slice(low * 2 * block, high * 2 * block)
        total = jnp.dot(enc[shard, :, some], msg[some, :], preferred_element_type=jnp.float32)
        if first:
            agg[...] = total
        else:
            agg[...] += total

    def poll(hop):
        @pl.when(line == hop + 1)
        def _():
            pl.semaphore_wait(ready.at[0], 1)
            pl.when(has_up)(functools.partial(tell, 0, up))

        @pl.when(line == lines - 2 - hop)
        def _():
            pl.semaphore_wait(ready.at[1], 1)
            pl.when(has_down)(functools.partial(tell, 1, down))

        known = by_line([max(at - 1, lines - 2 - at) for at in range(lines)]) == hop
        for source in range(lines):
            for its_side in range(2):
                near = jnp.where(side == its_side, jnp.abs(line - source), 2 * jnp.abs(line - source) + 1) <= 1
                pl.when(known & jnp.logical_not(near))(functools.partial(send_idx, source * 2 + its_side))

    poll(0)
    build_enc(me, wait=False)
    build_dec(me, wait=False)
    poll(1)
    for c in range(CHUNKS // 2, CHUNKS - 1):
        send_own(c)
    for copy in par_copies:
        copy.wait()
    w_src_all[...] = w_src_all[...] * 0.5
    bias_all[...] = bias_all[...] * 0.5
    encode(me, first=True)
    for hop in range(2, lines - 1):
        poll(hop)
    for c in range(CHUNKS - 1, CHUNKS):
        send_own(c)
    enc_tasks = [functools.partial(build_enc, shard) for shard in build_order[1:]]
    dec_tasks = [functools.partial(build_dec, shard, wait=False) for shard in build_order[1:]]
    tasks = [task for pair in zip(enc_tasks[:-2], dec_tasks[:-2]) for task in pair] + enc_tasks[-2:]
    dec_tasks = dec_tasks[-2:]

    def run(count):
        for _ in range(min(count, len(tasks))):
            tasks.pop(0)()

    def halves(c):
        return c >= CHUNKS // 2

    take_line, take_other, take_far = relays(x_part, x_send, xz_recv, xy_recv, halves, to_mate)
    def encodes(stage, parts):
        return [functools.partial(encode, shard, parts=parts) for at, shard in order if at == stage]

    run(2)
    for i in range(lines):
        for c in range(CHUNKS):
            if i < lines - 1:
                take_line(i, c, None)
            take_other(i, c)
            if i == lines - 2 and c == CHUNKS // 2:
                tasks.append(dec_tasks.pop(0))
                tasks += encodes(i, (0,))
            if i == lines - 1 and c == CHUNKS // 2:
                tasks += encodes(lines, (0,))
            run(1 + c // 2 if i == 0 else -(-len(tasks) // (CHUNKS - c)))
        tasks += encodes(i, (1,) if i == lines - 2 else (0, 1))
    for c in range(CHUNKS // 2, CHUNKS):
        take_far(c)
    run(len(tasks))
    for task in encodes(lines, (1,)):
        task()

    width = agg.shape[1] // 2
    my_first = pl.multiple_of(me * mesh_rows + core * half_mesh, half_mesh)

    def p_part(shard, q):
        flip, sub = q % 2, q // 2
        half = mate if flip else core
        first = shard * mesh_rows + half * half_mesh + sub * part_mesh
        return proj_all.at[pl.ds(pl.multiple_of(first, part_mesh), part_mesh)]

    for sub in range(SUBS):
        some = slice(sub * part_mesh, (sub + 1) * part_mesh)
        hidden = sum(
            jnp.dot(
                agg[some, h * width : (h + 1) * width].astype(jnp.bfloat16), w_node_all[h],
                preferred_element_type=jnp.float32,
            )
            for h in range(2)
        )
        projected = sum(
            jnp.dot(
                (
                    embed_all[h, some, :].astype(jnp.float32) + silu(hidden[:, h * width : (h + 1) * width])
                ).astype(jnp.bfloat16),
                w_dec_all[h], preferred_element_type=jnp.float32,
            )
            for h in range(2)
        ).astype(jnp.bfloat16)
        first_core = core == 0
        into = p_part(me, 2 * sub)
        proj_all[pl.ds(pl.multiple_of(my_first + sub * part_mesh, part_mesh), part_mesh), :] = jnp.where(
            first_core, projected[:, :cols], projected[:, cols:]
        )
        proj_mate[some, :] = jnp.where(first_core, projected[:, cols:], projected[:, :cols])
        for flip in range(2):
            ref = proj_mate.at[pl.ds(sub * part_mesh, part_mesh)] if flip else into
            chan = mate if flip else core
            for at, going, to, recv in (
                (UP, has_up, up, pz_recv), (DOWN, has_down, down, pz_recv), (ACROSS, None, other, py_recv),
            ):
                def go(ref=ref, into=into, at=at, to=to, recv=recv, q=2 * sub + flip, chan=chan):
                    remote(ref, into, p_send.at[at], recv.at[line, q], to, chan).start()
                if going is None:
                    go()
                else:
                    pl.when(going)(go)
    whole_half = proj_all.at[pl.ds(my_first, half_mesh)]
    remote(proj_mate, whole_half, p_send.at[MATE], pm_recv.at[0], me, mate).start()

    def decode(shard, first=False):
        remote(dec.at[0, pl.ds(0, half_grid)], dec.at[0, pl.ds(0, half_grid)], dec_send.at[0], dec_recv.at[shard], me, mate).wait_recv()
        rows = pl.ds(pl.multiple_of(shard * mesh_rows, mesh_rows), mesh_rows)
        for t in range(2):
            at = pl.ds(t * half_grid, half_grid)
            acc[at, :] += jnp.dot(dec[shard, at, :], proj_all[rows, :], preferred_element_type=jnp.float32)

    tasks = dec_tasks[:]
    take_line, take_other, take_far = relays(
        p_part, p_send, pz_recv, py_recv, lambda q: q >= SUBS, lambda shard, q: None)
    acc[...] = x_all[own_rows, pl.ds(pl.multiple_of(core * cols, cols), cols)].astype(jnp.float32)

    def own_decode():
        remote(proj_mate, whole_half, p_send.at[MATE], pm_recv.at[0], me, mate).wait_recv()
        decode(me)

    tasks.append(flush)
    pieces = 2 * SUBS
    while tasks:
        tasks.pop(0)()
    tasks.append(own_decode)
    for i in range(lines):
        if i < lines - 1:
            for q in range(pieces + 1):
                if q < pieces:
                    take_line(i, q, "inner")
                if q:
                    take_line(i, q - 1, "outer")
        for q in range(pieces):
            take_other(i, q)
            if tasks and i:
                tasks.pop(0)()
        while tasks and i == 0:
            tasks.pop(0)()
        tasks.extend(functools.partial(decode, shard) for stage, shard in order if stage == i)
    for q in range(SUBS, pieces):
        take_far(q)
    tasks.extend(functools.partial(decode, shard) for stage, shard in order if stage == lines)
    while tasks:
        tasks.pop(0)()
    out_ref[...] = acc[...].astype(jnp.bfloat16)

    def drained(ref, sem):
        remote(ref, ref, sem, sem, me, mate).wait_send()

    for at in range(lines):
        @pl.when(line == at)
        def _(at=at):
            for n, (x_n, p_n) in enumerate(zip(link_pieces(at, lines, CHUNKS), link_pieces(at, lines, pieces))):
                if x_n:
                    drained(x_all.at[pl.ds(0, x_n * block)], x_send.at[n])
                    drained(proj_all.at[pl.ds(0, p_n * part_mesh)], p_send.at[n])
    drained(x_all.at[pl.ds(0, (peers - 1) * half_grid)], x_send.at[MATE])
    drained(proj_mate, p_send.at[MATE])
    drained(idx_own.at[pl.ds(0, peers - 1)], idx_send.at[0])
    drained(dec.at[:, pl.ds(0, half_grid)], dec_send.at[0])


def fused(grid_state, w_src, bias_src, mesh_embed, w_node, w_dec, slot_src, slot_dst, slot_count):
    peers = lax.axis_size("graph")
    capacity = slot_src.shape[2]
    grid_rows, chans = grid_state.shape
    mesh_rows = mesh_embed.shape[0]
    hidden = w_src.shape[1]
    lines = peers // 2
    bf16, f32, i32 = jnp.bfloat16, jnp.float32, jnp.int32
    dma = pltpu.SemaphoreType.DMA
    pieces = 2 * SUBS
    return pl.pallas_call(
        functools.partial(graph_kernel, peers),
        out_shape=jax.ShapeDtypeStruct((grid_rows, chans // 2), bf16),
        in_specs=[pl.BlockSpec(memory_space=pl.ANY)] * 9,
        out_specs=pl.BlockSpec(memory_space=pltpu.VMEM),
        scratch_shapes=[
            pltpu.VMEM((peers * grid_rows, chans), bf16),
            pltpu.VMEM((peers, 2, capacity), i32),
            pltpu.VMEM((peers, 2, capacity), i32),
            pltpu.VMEM(slot_src.shape, i32),
            pltpu.VMEM(slot_dst.shape, i32),
            pltpu.SMEM(slot_count.shape, i32),
            pltpu.VMEM((2,) + w_src.shape, bf16),
            pltpu.VMEM((2, 1, hidden), f32),
            pltpu.VMEM((2, mesh_rows // 2, hidden), bf16),
            pltpu.VMEM((2,) + w_node.shape, bf16),
            pltpu.VMEM((2,) + w_dec.shape, bf16),
            pltpu.VMEM((peers, mesh_rows // 2, grid_rows), bf16),
            pltpu.VMEM((peers, grid_rows, mesh_rows), bf16),
            pltpu.VMEM((mesh_rows, capacity), HOT),
            pltpu.VMEM((grid_rows, 2 * hidden), bf16),
            pltpu.VMEM((mesh_rows // 2, 2 * hidden), f32),
            pltpu.VMEM((grid_rows, chans // 2), f32),
            pltpu.VMEM((mesh_rows // 2, chans // 2), bf16),
            pltpu.VMEM((peers * mesh_rows, chans // 2), bf16),
            pltpu.SemaphoreType.REGULAR((2,)),
            dma((9,)), dma((5,)), dma((5,)), dma((1,)), dma((peers,)),
            dma((4,)), dma((lines, CHUNKS)), dma((lines, CHUNKS)), dma((peers, 2)),
            dma((4,)), dma((lines, pieces)), dma((lines, pieces)), dma((1,)), dma((1,)), dma((peers,)),
        ],
        compiler_params=pltpu.CompilerParams(collective_id=0, has_side_effects=True),
    )(grid_state, w_src, bias_src[None, :], mesh_embed, w_node, w_dec, slot_src, slot_dst, slot_count)


def held_bytes(peers, grid_state, mesh_embed, *rest):
    grid_rows, chans = grid_state.shape
    mesh_rows = mesh_embed.shape[0]
    return 2 * peers * grid_rows * (chans + 2 * mesh_rows)


def per_device(grid_state, w_src, bias_src, mesh_embed, *rest):
    peers = lax.axis_size("graph")
    fits = (
        peers % 2 == 0
        and peers >= 4
        and lax.axis_size("chan") == 2
        and held_bytes(peers, grid_state, mesh_embed) <= VMEM_BUDGET
    )
    body = fused if fits else on_device
    return body(grid_state, w_src, bias_src, mesh_embed, *rest)


def solution(mesh):
    placed = (
        P(("member", "graph"), None),
        P(None, "chan"),
        P("chan"),
        P("graph", "chan"),
        P("chan", None),
        P("chan", None),
        P("graph", None, None),
        P(None, "graph", None),
        P(),
    )
    return jax.shard_map(
        per_device,
        mesh=mesh,
        in_specs=placed,
        out_specs=P(("member", "graph"), "chan"),
        check_vma=False,
    )
```

```python
import functools
import math

import jax
import jax.numpy as jnp
from jax import lax
from jax.experimental import pallas as pl
from jax.experimental.pallas import tpu as pltpu
from jax.sharding import PartitionSpec as P

CHUNKS = 4
SUBS = 2
HOT = jnp.float8_e4m3fn
VMEM_BUDGET = 48 * 2**20
MESH = pl.DeviceIdType.MESH
NT = (((1,), (1,)), ((), ()))


def edge_network(source_rows, w_src, bias_src):
    return jax.nn.silu(
        jnp.dot(source_rows, w_src, preferred_element_type=jnp.float32) + bias_src
    ).astype(jnp.bfloat16)


def segment_rows(values, indices, usable, row_count):
    slot_total = values.shape[0]
    width = values.shape[1]
    block_len = math.gcd(slot_total, 2048)
    block_count = slot_total // block_len
    targets = jnp.where(usable, indices, -1).reshape(block_count, block_len)
    pieces = values.reshape(block_count, block_len, width)
    row_ids = jnp.arange(row_count, dtype=jnp.int32)

    def add_block(summed, scan_item):
        row_target, piece_vals = scan_item
        one_hot = (row_ids[:, None] == row_target[None, :]).astype(jnp.bfloat16)
        return (summed + jnp.dot(one_hot, piece_vals, preferred_element_type=jnp.float32), None)

    result, unused = lax.scan(
        add_block, jnp.zeros((row_count, width), jnp.float32), (targets, pieces)
    )
    return result


def on_device(
    grid_state, w_src, bias_src, mesh_embed, w_node, w_dec, slot_src, slot_dst, slot_count
):
    peers = lax.axis_size("graph")
    own_index = lax.axis_index("graph")
    core_index = lax.axis_index("chan")
    capacity = slot_src.shape[2]
    positions = jnp.arange(capacity, dtype=jnp.int32)
    grid_rows = grid_state.shape[0]
    mesh_rows = mesh_embed.shape[0]
    sent_counts = lax.dynamic_slice_in_dim(slot_count, own_index, 1, 0)[0]
    recv_counts = lax.dynamic_slice_in_dim(slot_count, own_index, 1, 1)[:, 0]
    half_slots = capacity // 2
    chosen = lax.dynamic_slice_in_dim(slot_src[0], core_index * half_slots, half_slots, 1)
    picked = jnp.take(grid_state, chosen.reshape(-1), axis=0).reshape(
        peers, half_slots, grid_state.shape[1]
    )
    arrived = lax.all_to_all(picked, "graph", split_axis=0, concat_axis=0, tiled=True)
    joined = lax.all_gather(arrived, "chan", axis=1, tiled=True)
    messages = edge_network(joined.reshape(peers * capacity, grid_state.shape[1]), w_src, bias_src)
    arrive_ok = (positions[None, :] < recv_counts[:, None]).reshape(-1)
    dst_rows = slot_dst[:, 0, :].reshape(-1)
    aggregate = segment_rows(messages, dst_rows, arrive_ok, mesh_rows)
    partial_hidden = jnp.dot(
        aggregate.astype(jnp.bfloat16), w_node, preferred_element_type=jnp.float32
    )
    hidden_pre = lax.psum_scatter(partial_hidden, "chan", scatter_dimension=1, tiled=True)
    latent = (mesh_embed.astype(jnp.float32) + jax.nn.silu(hidden_pre)).astype(jnp.bfloat16)
    partial_proj = jnp.dot(latent, w_dec, preferred_element_type=jnp.float32)
    projected = lax.psum_scatter(partial_proj, "chan", scatter_dimension=1, tiled=True).astype(
        jnp.bfloat16
    )
    returned = jnp.take(projected, dst_rows, axis=0).reshape(peers, capacity, projected.shape[1])
    came_back = lax.all_to_all(returned, "graph", split_axis=0, concat_axis=0, tiled=True).reshape(
        peers * capacity, projected.shape[1]
    )
    send_ok = (positions[None, :] < sent_counts[:, None]).reshape(-1)
    decoded = segment_rows(came_back, slot_src[0].reshape(-1), send_ok, grid_rows)
    width_half = decoded.shape[1]
    own_cols = lax.dynamic_slice_in_dim(grid_state, core_index * width_half, width_half, 1)
    return (own_cols.astype(jnp.float32) + decoded).astype(jnp.bfloat16)


def silu(v):
    half = 0.5 * v
    return half + half * jnp.tanh(half)


def one_hot(first, rows, indices):
    row_ids = lax.broadcasted_iota(jnp.int16, (rows, indices.shape[1]), 0)
    hits = row_ids == (indices - first).astype(jnp.int16)
    return jnp.where(hits, jnp.bfloat16(1), jnp.bfloat16(0)).astype(HOT)


def is_end(line, lines):
    return line in (0, lines - 1)


def given(line, lines):
    outer = line - 1 if line < lines // 2 else line + 1
    return outer if not is_end(line, lines) and is_end(outer, lines) else None


def arrival_order(line, lines):
    stages = [(0, 1, 0, line)]
    for source in range(lines):
        gap = abs(source - line)
        if gap:
            split = is_end(line, lines) and gap > 1
            stages += [(gap - 1, 0, gap, source), (lines if split else gap, 1, gap, source)]
    return sorted(stages)


def link_pieces(line, lines, pieces):
    def extra(to):
        if not 0 <= to < lines:
            return 0
        return lines - 2 if is_end(to, lines) else pieces if given(to, lines) == line else 0

    up = pieces * (line + 1) + extra(line + 1) if line < lines - 1 else 0
    down = pieces * (lines - line) + extra(line - 1) if line > 0 else 0
    across = pieces * lines
    if given(line, lines) is not None:
        across -= pieces
    if is_end(line, lines):
        across -= lines - 2
    return up, down, across


def return_order(line, lines):
    stages = [(0, 1, 0, line)]
    for source in range(lines):
        gap = abs(source - line)
        if gap:
            stages += [(gap - 1, 0, gap, source), (lines - 2 + gap, 1, gap, source)]
    return sorted(stages)


def return_pieces(line, lines, pieces):
    direct = lines > 2

    def one_way(to, behind, first):
        if not 0 <= to < lines:
            return 0
        onward = behind - (1 if direct and is_end(to, lines) and behind else 0)
        beside = pieces // 2 if is_end(to, lines) else pieces if given(to, lines) == line else 0
        return pieces * (1 + (1 if direct and first else 0) + onward) + beside

    up = one_way(line + 1, line, line == 0)
    down = one_way(line - 1, lines - 1 - line, line == lines - 1)
    skipped = pieces if given(line, lines) is not None else pieces // 2 if is_end(line, lines) else 0
    return up, down, pieces * lines - skipped


def graph_kernel(
    peers,
    x_ref, w_src_ref, bias_ref, embed_ref, w_node_ref, w_dec_ref, src_ref, dst_ref, count_ref,
    out_ref,
    x_all, idx_own, idx_in, src_vmem, dst_vmem, count_smem, w_src_all, bias_all, embed_all, w_node_all, w_dec_all,
    enc, dec, hot, msg, agg, acc, proj_mate, proj_all,
    ready, local_sem, par_send, par_recv, idx_send, idx_recv,
    x_send, xz_recv, xy_recv, xm_recv, p_send, pz_recv, py_recv, pm_recv, dec_send, dec_recv,
):
    lines = peers // 2
    me = lax.axis_index("graph")
    core = lax.axis_index("chan")
    mate = 1 - core
    line, side = me // 2, me % 2
    other = line * 2 + (1 - side)
    up, down = (line + 1) * 2 + side, (line - 1) * 2 + side
    has_up, has_down = line < lines - 1, line > 0
    low_half = line < lines // 2
    grid_rows, chans = x_ref.shape
    half_grid = grid_rows // 2
    block = half_grid // CHUNKS
    mesh_rows = embed_ref.shape[0]
    half_mesh = mesh_rows // 2
    part_mesh = half_mesh // SUBS
    cols = chans // 2
    capacity = src_ref.shape[2]
    UP, DOWN, ACROSS, MATE = range(4)

    def remote(src, dst, send, recv, graph, chan):
        return pltpu.make_async_remote_copy(
            src_ref=src, dst_ref=dst, send_sem=send, recv_sem=recv,
            device_id={"graph": graph, "chan": chan}, device_id_type=MESH,
        )

    def by_line(values):
        return sum(jnp.where(line == at, values[at], 0) for at in range(lines))

    end = (line == 0) | (line == lines - 1)
    giver = by_line([-1 if given(at, lines) is None else given(at, lines) for at in range(lines)])
    barrier = pltpu.get_barrier_semaphore()

    def greet(graph, chan):
        pl.semaphore_signal(barrier, inc=1, device_id={"graph": graph, "chan": chan}, device_id_type=MESH)

    greet(me, mate)
    for chan in (core, mate):
        greet(other, chan)
        pl.when(has_up)(functools.partial(greet, up, chan))
        pl.when(has_down)(functools.partial(greet, down, chan))
    my_rows = pl.ds(pl.multiple_of(core * half_mesh, half_mesh), half_mesh)
    mate_rows = pl.ds(pl.multiple_of(mate * half_mesh, half_mesh), half_mesh)
    own_rows = pl.ds(pl.multiple_of(me * grid_rows, grid_rows), grid_rows)
    locals_ = [
        pltpu.make_async_copy(src_ref, src_vmem, local_sem.at[0]),
        pltpu.make_async_copy(dst_ref, dst_vmem, local_sem.at[1]),
        pltpu.make_async_copy(count_ref, count_smem, local_sem.at[2]),
        pltpu.make_async_copy(x_ref, x_all.at[own_rows], local_sem.at[3]),
        pltpu.make_async_copy(w_src_ref, w_src_all.at[core], local_sem.at[4]),
        pltpu.make_async_copy(bias_ref, bias_all.at[core], local_sem.at[5]),
        pltpu.make_async_copy(w_node_ref, w_node_all.at[core], local_sem.at[6]),
        pltpu.make_async_copy(w_dec_ref, w_dec_all.at[core], local_sem.at[7]),
        pltpu.make_async_copy(embed_ref.at[my_rows], embed_all.at[core], local_sem.at[8]),
    ]
    for copy in locals_[3:4] + locals_[:3] + locals_[4:]:
        copy.start()
    locals_[3].wait()
    pl.semaphore_wait(barrier, 3 + 2 * jnp.where(has_up, 1, 0) + 2 * jnp.where(has_down, 1, 0))

    def x_part(shard, c, half=core):
        first = shard * grid_rows + c * 2 * block + half * block
        return x_all.at[pl.ds(pl.multiple_of(first, block), block)]

    def send_own(c):
        ref = x_part(me, c)
        for at, going, to, recv in (
            (UP, has_up, up, xz_recv), (DOWN, has_down, down, xz_recv), (ACROSS, None, other, xy_recv),
        ):
            def go(at=at, to=to, recv=recv):
                remote(ref, ref, x_send.at[at], recv.at[line, c], to, core).start()
            if going is None:
                go()
            else:
                pl.when(going)(go)

    send_own(0)
    for copy in locals_[:3]:
        copy.wait()
    slots = lax.broadcasted_iota(jnp.int32, (1, capacity), 1)
    for to in range(peers):
        idx_own[to, 0:1, :] = jnp.where(slots < count_smem[me, to], src_vmem[0, to : to + 1, :], -1)
        idx_own[to, 1:2, :] = dst_vmem[to]
    idx_in[me] = idx_own[me]

    def send_idx(to):
        remote(idx_own.at[to], idx_in.at[me], idx_send.at[0], idx_recv.at[me], to, core).start()

    send_idx(other)
    pl.when(has_up)(functools.partial(send_idx, up))
    pl.when(has_down)(functools.partial(send_idx, down))
    for c in range(1, CHUNKS - 1):
        send_own(c)
    for copy in locals_[4:]:
        copy.wait()
    par_copies = [
        remote(w_src_all.at[core], w_src_all.at[core], par_send.at[0], par_recv.at[0], me, mate),
        remote(bias_all.at[core], bias_all.at[core], par_send.at[1], par_recv.at[1], me, mate),
        remote(embed_ref.at[mate_rows], embed_all.at[core], par_send.at[2], par_recv.at[2], me, mate),
        remote(w_node_all.at[core], w_node_all.at[core], par_send.at[3], par_recv.at[3], me, mate),
        remote(w_dec_all.at[core], w_dec_all.at[core], par_send.at[4], par_recv.at[4], me, mate),
    ]
    for copy in par_copies:
        copy.start()

    def tell(at, to):
        pl.semaphore_signal(ready.at[at], inc=1, device_id={"graph": to, "chan": core}, device_id_type=MESH)

    pl.when(line == 0)(functools.partial(tell, 0, up))
    pl.when(line == lines - 1)(functools.partial(tell, 1, down))

    def relays(part, send, z_recv, y_recv, late, arrived, back=False):
        def extra(source, q, above):
            ref = part(source * 2 + 1 - side, q)
            remote(ref, ref, send.at[UP if above else DOWN], y_recv.at[source, q], up if above else down, core).start()

        def extras(source, q):
            for above, there in ((True, has_up), (False, has_down)):
                to = line + 1 if above else line - 1
                to_end = (to == 0) | (to == lines - 1)
                to_giver = by_line([
                    -1 if not 0 <= at + (1 if above else -1) < lines
                    or given(at + (1 if above else -1), lines) is None
                    else given(at + (1 if above else -1), lines)
                    for at in range(lines)
                ])
                wanted = (source == line) & (to_giver == line)
                if back:
                    wanted = (source == line) & ((to_giver == line) | to_end) if late(q) else wanted
                elif late(q):
                    wanted = wanted | (to_end & (jnp.abs(source - to) > 1))
                pl.when(there & wanted)(functools.partial(extra, source, q, above))

        def take_line(i, q, which):
            for above in (True, False):
                source = line + 1 + i if above else line - 1 - i
                valid = (source < lines) if above else (source >= 0)
                if which is not None:
                    valid = valid & ((low_half if above else jnp.logical_not(low_half)) == (which == "inner"))
                onward, to, at = (has_down, down, DOWN) if above else (has_up, up, UP)

                @pl.when(valid)
                def _(source=source, onward=onward, to=to, at=at):
                    ref = part(source * 2 + side, q)
                    remote(ref, ref, send.at[at], z_recv.at[source, q], me, mate).wait_recv()

                    if back and lines > 2:
                        to_line = line - 1 if above else line + 1
                        onward = onward & ((to_line != (0 if above else lines - 1)) | (source != (lines - 1 if above else 0)))

                    @pl.when(onward)
                    def _():
                        remote(ref, ref, send.at[at], z_recv.at[source, q], to, core).start()

                    crossing = source != giver
                    if late(q):
                        gap_of = jnp.abs(source - line)
                        crossing = crossing & jnp.logical_not(end & ((gap_of == 1) if back else (gap_of > 1)))

                    @pl.when(crossing)
                    def _():
                        remote(ref, ref, send.at[ACROSS], y_recv.at[source, q], other, core).start()

                    arrived(source * 2 + side, q)

        def take_other(i, q):
            def take(source):
                shard = source * 2 + 1 - side
                ref = part(shard, q)
                remote(ref, ref, send.at[ACROSS], y_recv.at[source, q], me, mate).wait_recv()
                extras(source, q)
                arrived(shard, q)

            if i == 0:
                take(line)
                return
            for source, valid in ((line + i, line + i < lines), (line - i, line - i >= 0)):
                if late(q) and not back and i > 1:
                    valid = valid & jnp.logical_not(end)
                pl.when(valid)(functools.partial(take, source))

        def take_far(i, q):
            pl.when(end)(functools.partial(take_one, jnp.where(low_half, line + i, line - i), q))

        def take_one(source, q):
            shard = source * 2 + 1 - side
            ref = part(shard, q)
            remote(ref, ref, send.at[ACROSS], y_recv.at[source, q], me, mate).wait_recv()
            arrived(shard, q)

        return take_line, take_other, take_far

    def to_mate(shard, c):
        ref = x_part(shard, c)
        remote(ref, ref, x_send.at[MATE], xm_recv.at[shard, c // (CHUNKS // 2)], me, mate).start()

    nearest = [sorted((p for p in range(lines) if p != at), key=lambda p: (abs(p - at), p)) for at in range(lines)]
    build_order = [me, other]
    for i in range(lines - 1):
        source = by_line([nearest[at][i] for at in range(lines)])
        build_order += [source * 2 + side, source * 2 + 1 - side]

    def by_stage(rule):
        tables = [rule(at, lines) for at in range(lines)]
        found = []
        for k in range(peers - 1):
            source = by_line([tables[at][k][3] for at in range(lines)])
            flip = by_line([tables[at][k][1] for at in range(lines)])
            stage = max(tables[at][k][0] for at in range(lines))
            found.append((stage, source * 2 + jnp.where(flip == 1, 1 - side, side)))
        return found

    order, order_back = by_stage(arrival_order), by_stage(return_order)

    def build_enc(shard, wait=True):
        if wait:
            remote(idx_own.at[0], idx_in.at[shard], idx_send.at[0], idx_recv.at[shard], me, mate).wait_recv()
        hot[:half_mesh, :] = one_hot(core * half_mesh, half_mesh, dst_vmem[shard])
        for t in range(2):
            picks = one_hot(t * half_grid, half_grid, idx_in[shard, 0:1, :])
            enc[shard, :, t * half_grid : (t + 1) * half_grid] = lax.dot_general(
                hot[:half_mesh, :], picks, NT, preferred_element_type=jnp.float32
            ).astype(jnp.bfloat16)

    pending = []

    def dec_copy(shard, half):
        ref = dec.at[shard, pl.ds(pl.multiple_of(half * half_grid, half_grid), half_grid)]
        return remote(ref, ref, dec_send.at[0], dec_recv.at[shard], me, mate)

    def flush():
        while pending:
            dec_copy(pending.pop(0), core).start()

    def build_dec(shard, wait=True):
        flush()
        hot[...] = one_hot(0, mesh_rows, idx_in[shard, 1:2, :])
        for t in range(half_grid // 256):
            first = pl.multiple_of(core * half_grid, half_grid) + t * 256
            picks = one_hot(first, 256, idx_own[shard, 0:1, :])
            dec[shard, pl.ds(pl.multiple_of(first, 256), 256), :] = lax.dot_general(
                picks, hot[...], NT, preferred_element_type=jnp.float32
            ).astype(jnp.bfloat16)
        pending.append(shard)

    def encode(shard, first=False, parts=(0, 1)):
        if not first:
            for part in parts:
                some = x_all.at[pl.ds(0, half_grid // 2)]
                remote(some, some, x_send.at[MATE], xm_recv.at[shard, part], me, mate).wait_recv()
        low, high = min(parts) * CHUNKS // 2, (max(parts) + 1) * CHUNKS // 2
        for c in range(low, high):
            rows = pl.ds(pl.multiple_of(shard * grid_rows, grid_rows) + c * 2 * block, 2 * block)
            for h in range(2):
                pre = jnp.dot(x_all[rows, :], w_src_all[h], preferred_element_type=jnp.float32) + bias_all[h]
                msg[c * 2 * block : (c + 1) * 2 * block, h * (msg.shape[1] // 2) : (h + 1) * (msg.shape[1] // 2)] = (
                    pre + pre * jnp.tanh(pre)
                ).astype(jnp.bfloat16)
        some = slice(low * 2 * block, high * 2 * block)
        total = jnp.dot(enc[shard, :, some], msg[some, :], preferred_element_type=jnp.float32)
        if first:
            agg[...] = total
        else:
            agg[...] += total

    def poll(hop):
        @pl.when(line == hop + 1)
        def _():
            pl.semaphore_wait(ready.at[0], 1)
            pl.when(has_up)(functools.partial(tell, 0, up))

        @pl.when(line == lines - 2 - hop)
        def _():
            pl.semaphore_wait(ready.at[1], 1)
            pl.when(has_down)(functools.partial(tell, 1, down))

        known = by_line([max(at - 1, lines - 2 - at) for at in range(lines)]) == hop
        for source in range(lines):
            for its_side in range(2):
                near = jnp.where(side == its_side, jnp.abs(line - source), 2 * jnp.abs(line - source) + 1) <= 1
                pl.when(known & jnp.logical_not(near))(functools.partial(send_idx, source * 2 + its_side))

    poll(0)
    build_enc(me, wait=False)
    build_dec(me, wait=False)
    poll(1)
    for copy in par_copies:
        copy.wait()
    w_src_all[...] = w_src_all[...] * 0.5
    bias_all[...] = bias_all[...] * 0.5
    encode(me, first=True)
    for hop in range(2, lines - 1):
        poll(hop)
    for c in range(CHUNKS - 1, CHUNKS):
        send_own(c)
    enc_tasks = [functools.partial(build_enc, shard) for shard in build_order[1:]]
    dec_tasks = [functools.partial(build_dec, shard, wait=False) for shard in build_order[1:]]
    tasks = [task for pair in zip(enc_tasks[:-2], dec_tasks[:-2]) for task in pair] + enc_tasks[-2:]
    dec_tasks = dec_tasks[-2:]

    def run(count):
        for _ in range(min(count, len(tasks))):
            tasks.pop(0)()

    def halves(c):
        return c == CHUNKS - 1

    take_line, take_other, take_far = relays(x_part, x_send, xz_recv, xy_recv, halves, to_mate)
    def encodes(stage, parts):
        return [functools.partial(encode, shard, parts=parts) for at, shard in order if at == stage]

    run(2)
    for i in range(lines - 1):
        for c in range(CHUNKS):
            take_line(i, c, None)
            take_other(i, c)
            if i == lines - 2 and c == CHUNKS // 2:
                tasks += encodes(i, (0,))
            run(1 + c // 2 if i == 0 else -(-len(tasks) // (CHUNKS - c)))
        tasks += encodes(i, (0, 1) if i < lines - 2 else (1,))
        if i == lines - 3:
            tasks[1:1] = dec_tasks[:1]
            tasks += dec_tasks[1:]
            del dec_tasks[:]
    tasks += encodes(lines, (0,))
    for c in range(CHUNKS - 1):
        take_other(lines - 1, c)
        if c == CHUNKS - 2:
            for gap in range(2, lines - 1):
                take_far(gap, CHUNKS - 1)
        run(-(-len(tasks) // (CHUNKS - 1 - c)))
    if lines > 2:
        take_far(lines - 1, CHUNKS - 1)
    for task in encodes(lines, (1,)):
        task()

    width = agg.shape[1] // 2
    my_first = pl.multiple_of(me * mesh_rows + core * half_mesh, half_mesh)

    def p_part(shard, q):
        flip, sub = q % 2, q // 2
        half = mate if flip else core
        first = shard * mesh_rows + half * half_mesh + sub * part_mesh
        return proj_all.at[pl.ds(pl.multiple_of(first, part_mesh), part_mesh)]

    for sub in range(SUBS):
        some = slice(sub * part_mesh, (sub + 1) * part_mesh)
        hidden = sum(
            jnp.dot(
                agg[some, h * width : (h + 1) * width].astype(jnp.bfloat16), w_node_all[h],
                preferred_element_type=jnp.float32,
            )
            for h in range(2)
        )
        projected = sum(
            jnp.dot(
                (
                    embed_all[h, some, :].astype(jnp.float32) + silu(hidden[:, h * width : (h + 1) * width])
                ).astype(jnp.bfloat16),
                w_dec_all[h], preferred_element_type=jnp.float32,
            )
            for h in range(2)
        ).astype(jnp.bfloat16)
        first_core = core == 0
        into = p_part(me, 2 * sub)
        proj_all[pl.ds(pl.multiple_of(my_first + sub * part_mesh, part_mesh), part_mesh), :] = jnp.where(
            first_core, projected[:, :cols], projected[:, cols:]
        )
        proj_mate[some, :] = jnp.where(first_core, projected[:, cols:], projected[:, :cols])
        for flip in range(2):
            ref = proj_mate.at[pl.ds(sub * part_mesh, part_mesh)] if flip else into
            chan = mate if flip else core
            routes = [(UP, has_up, up, pz_recv), (DOWN, has_down, down, pz_recv), (ACROSS, None, other, py_recv)]
            if lines > 2:
                routes[:0] = [
                    (UP, line == 0, (lines - 1) * 2 + side, pz_recv), (DOWN, line == lines - 1, side, pz_recv),
                ]
            for at, going, to, recv in routes:
                def go(ref=ref, into=into, at=at, to=to, recv=recv, q=2 * sub + flip, chan=chan):
                    remote(ref, into, p_send.at[at], recv.at[line, q], to, chan).start()
                if going is None:
                    go()
                else:
                    pl.when(going)(go)
    whole_half = proj_all.at[pl.ds(my_first, half_mesh)]
    remote(proj_mate, whole_half, p_send.at[MATE], pm_recv.at[0], me, mate).start()

    def decode(*shards):
        some = dec.at[0, pl.ds(0, half_grid)]
        for shard in shards:
            remote(some, some, dec_send.at[0], dec_recv.at[shard], me, mate).wait_recv()
        for t in range(2):
            at = pl.ds(t * half_grid, half_grid)
            acc[at, :] += sum(
                jnp.dot(
                    dec[shard, at, :], proj_all[pl.ds(pl.multiple_of(shard * mesh_rows, mesh_rows), mesh_rows), :],
                    preferred_element_type=jnp.float32,
                )
                for shard in shards
            )

    take_line, take_other, _ = relays(
        p_part, p_send, pz_recv, py_recv, lambda q: q >= SUBS, lambda shard, q: None, back=True)
    acc[...] = x_all[own_rows, pl.ds(pl.multiple_of(core * cols, cols), cols)].astype(jnp.float32)

    def own_decode():
        remote(proj_mate, whole_half, p_send.at[MATE], pm_recv.at[0], me, mate).wait_recv()
        decode(me)

    pieces = 2 * SUBS
    flush()
    tasks.append(own_decode)

    for q in range(pieces):
        take_line(0, q, "inner")
        if q:
            take_other(0, q - 1)
    take_other(0, pieces - 1)
    for q in range(pieces):
        take_line(0, q, "outer")
    for q in range(pieces):
        for i in range(1, lines - 1):
            take_line(i, q, "inner")
            take_line(i, q, "outer")
        if q % 2:
            run(1)
    run(len(tasks))
    early = [shard for at, shard in order_back if at < lines - 1]
    for n in range(0, len(early), 2):
        decode(*early[n : n + 2])
    for q in range(pieces):
        for i in range(1, lines):
            if i > 1 or q < SUBS:
                take_other(i, q)
        if q == pieces - 2:
            for late_q in range(SUBS, pieces):
                take_other(1, late_q)
            for at, shard in order_back:
                if at == lines - 1:
                    decode(shard)
    final = [shard for at, shard in order_back if at >= lines]
    if final:
        decode(*final)
    out_ref[...] = acc[...].astype(jnp.bfloat16)

    def drained(ref, sem):
        remote(ref, ref, sem, sem, me, mate).wait_send()

    for at in range(lines):
        @pl.when(line == at)
        def _(at=at):
            for n, (x_n, p_n) in enumerate(zip(link_pieces(at, lines, CHUNKS), return_pieces(at, lines, pieces))):
                if x_n:
                    drained(x_all.at[pl.ds(0, x_n * block)], x_send.at[n])
                    drained(proj_all.at[pl.ds(0, p_n * part_mesh)], p_send.at[n])
    drained(x_all.at[pl.ds(0, (peers - 1) * half_grid)], x_send.at[MATE])
    drained(proj_mate, p_send.at[MATE])
    drained(idx_own.at[pl.ds(0, peers - 1)], idx_send.at[0])
    drained(dec.at[:, pl.ds(0, half_grid)], dec_send.at[0])


def fused(grid_state, w_src, bias_src, mesh_embed, w_node, w_dec, slot_src, slot_dst, slot_count):
    peers = lax.axis_size("graph")
    capacity = slot_src.shape[2]
    grid_rows, chans = grid_state.shape
    mesh_rows = mesh_embed.shape[0]
    hidden = w_src.shape[1]
    lines = peers // 2
    bf16, f32, i32 = jnp.bfloat16, jnp.float32, jnp.int32
    dma = pltpu.SemaphoreType.DMA
    pieces = 2 * SUBS
    return pl.pallas_call(
        functools.partial(graph_kernel, peers),
        out_shape=jax.ShapeDtypeStruct((grid_rows, chans // 2), bf16),
        in_specs=[pl.BlockSpec(memory_space=pl.ANY)] * 9,
        out_specs=pl.BlockSpec(memory_space=pltpu.VMEM),
        scratch_shapes=[
            pltpu.VMEM((peers * grid_rows, chans), bf16),
            pltpu.VMEM((peers, 2, capacity), i32),
            pltpu.VMEM((peers, 2, capacity), i32),
            pltpu.VMEM(slot_src.shape, i32),
            pltpu.VMEM(slot_dst.shape, i32),
            pltpu.SMEM(slot_count.shape, i32),
            pltpu.VMEM((2,) + w_src.shape, bf16),
            pltpu.VMEM((2, 1, hidden), f32),
            pltpu.VMEM((2, mesh_rows // 2, hidden), bf16),
            pltpu.VMEM((2,) + w_node.shape, bf16),
            pltpu.VMEM((2,) + w_dec.shape, bf16),
            pltpu.VMEM((peers, mesh_rows // 2, grid_rows), bf16),
            pltpu.VMEM((peers, grid_rows, mesh_rows), bf16),
            pltpu.VMEM((mesh_rows, capacity), HOT),
            pltpu.VMEM((grid_rows, 2 * hidden), bf16),
            pltpu.VMEM((mesh_rows // 2, 2 * hidden), f32),
            pltpu.VMEM((grid_rows, chans // 2), f32),
            pltpu.VMEM((mesh_rows // 2, chans // 2), bf16),
            pltpu.VMEM((peers * mesh_rows, chans // 2), bf16),
            pltpu.SemaphoreType.REGULAR((2,)),
            dma((9,)), dma((5,)), dma((5,)), dma((1,)), dma((peers,)),
            dma((4,)), dma((lines, CHUNKS)), dma((lines, CHUNKS)), dma((peers, 2)),
            dma((4,)), dma((lines, pieces)), dma((lines, pieces)), dma((1,)), dma((1,)), dma((peers,)),
        ],
        compiler_params=pltpu.CompilerParams(collective_id=0, has_side_effects=True),
    )(grid_state, w_src, bias_src[None, :], mesh_embed, w_node, w_dec, slot_src, slot_dst, slot_count)


def held_bytes(peers, grid_state, mesh_embed, *rest):
    grid_rows, chans = grid_state.shape
    mesh_rows = mesh_embed.shape[0]
    return 2 * peers * grid_rows * (chans + 2 * mesh_rows)


def per_device(grid_state, w_src, bias_src, mesh_embed, *rest):
    peers = lax.axis_size("graph")
    fits = (
        peers % 2 == 0
        and peers >= 4
        and lax.axis_size("chan") == 2
        and held_bytes(peers, grid_state, mesh_embed) <= VMEM_BUDGET
    )
    body = fused if fits else on_device
    return body(grid_state, w_src, bias_src, mesh_embed, *rest)


def solution(mesh):
    placed = (
        P(("member", "graph"), None),
        P(None, "chan"),
        P("chan"),
        P("graph", "chan"),
        P("chan", None),
        P("chan", None),
        P("graph", None, None),
        P(None, "graph", None),
        P(),
    )
    return jax.shard_map(
        per_device,
        mesh=mesh,
        in_specs=placed,
        out_specs=P(("member", "graph"), "chan"),
        check_vma=False,
    )
```

```python
import functools
import math

import jax
import jax.numpy as jnp
from jax import lax
from jax.experimental import pallas as pl
from jax.experimental.pallas import tpu as pltpu
from jax.sharding import PartitionSpec as P

CHUNKS = 4
SUBS = 2
EARLY = 1
HOT = jnp.float8_e4m3fn
VMEM_BUDGET = 48 * 2**20
MESH = pl.DeviceIdType.MESH
NT = (((1,), (1,)), ((), ()))


def edge_network(source_rows, w_src, bias_src):
    return jax.nn.silu(
        jnp.dot(source_rows, w_src, preferred_element_type=jnp.float32) + bias_src
    ).astype(jnp.bfloat16)


def segment_rows(values, indices, usable, row_count):
    slot_total = values.shape[0]
    width = values.shape[1]
    block_len = math.gcd(slot_total, 2048)
    block_count = slot_total // block_len
    targets = jnp.where(usable, indices, -1).reshape(block_count, block_len)
    pieces = values.reshape(block_count, block_len, width)
    row_ids = jnp.arange(row_count, dtype=jnp.int32)

    def add_block(summed, scan_item):
        row_target, piece_vals = scan_item
        one_hot = (row_ids[:, None] == row_target[None, :]).astype(jnp.bfloat16)
        return (summed + jnp.dot(one_hot, piece_vals, preferred_element_type=jnp.float32), None)

    result, unused = lax.scan(
        add_block, jnp.zeros((row_count, width), jnp.float32), (targets, pieces)
    )
    return result


def on_device(
    grid_state, w_src, bias_src, mesh_embed, w_node, w_dec, slot_src, slot_dst, slot_count
):
    peers = lax.axis_size("graph")
    own_index = lax.axis_index("graph")
    core_index = lax.axis_index("chan")
    capacity = slot_src.shape[2]
    positions = jnp.arange(capacity, dtype=jnp.int32)
    grid_rows = grid_state.shape[0]
    mesh_rows = mesh_embed.shape[0]
    sent_counts = lax.dynamic_slice_in_dim(slot_count, own_index, 1, 0)[0]
    recv_counts = lax.dynamic_slice_in_dim(slot_count, own_index, 1, 1)[:, 0]
    half_slots = capacity // 2
    chosen = lax.dynamic_slice_in_dim(slot_src[0], core_index * half_slots, half_slots, 1)
    picked = jnp.take(grid_state, chosen.reshape(-1), axis=0).reshape(
        peers, half_slots, grid_state.shape[1]
    )
    arrived = lax.all_to_all(picked, "graph", split_axis=0, concat_axis=0, tiled=True)
    joined = lax.all_gather(arrived, "chan", axis=1, tiled=True)
    messages = edge_network(joined.reshape(peers * capacity, grid_state.shape[1]), w_src, bias_src)
    arrive_ok = (positions[None, :] < recv_counts[:, None]).reshape(-1)
    dst_rows = slot_dst[:, 0, :].reshape(-1)
    aggregate = segment_rows(messages, dst_rows, arrive_ok, mesh_rows)
    partial_hidden = jnp.dot(
        aggregate.astype(jnp.bfloat16), w_node, preferred_element_type=jnp.float32
    )
    hidden_pre = lax.psum_scatter(partial_hidden, "chan", scatter_dimension=1, tiled=True)
    latent = (mesh_embed.astype(jnp.float32) + jax.nn.silu(hidden_pre)).astype(jnp.bfloat16)
    partial_proj = jnp.dot(latent, w_dec, preferred_element_type=jnp.float32)
    projected = lax.psum_scatter(partial_proj, "chan", scatter_dimension=1, tiled=True).astype(
        jnp.bfloat16
    )
    returned = jnp.take(projected, dst_rows, axis=0).reshape(peers, capacity, projected.shape[1])
    came_back = lax.all_to_all(returned, "graph", split_axis=0, concat_axis=0, tiled=True).reshape(
        peers * capacity, projected.shape[1]
    )
    send_ok = (positions[None, :] < sent_counts[:, None]).reshape(-1)
    decoded = segment_rows(came_back, slot_src[0].reshape(-1), send_ok, grid_rows)
    width_half = decoded.shape[1]
    own_cols = lax.dynamic_slice_in_dim(grid_state, core_index * width_half, width_half, 1)
    return (own_cols.astype(jnp.float32) + decoded).astype(jnp.bfloat16)


def silu(v):
    half = 0.5 * v
    return half + half * jnp.tanh(half)


def one_hot(first, rows, indices):
    row_ids = lax.broadcasted_iota(jnp.int16, (rows, indices.shape[1]), 0)
    hits = row_ids == (indices - first).astype(jnp.int16)
    return jnp.where(hits, jnp.bfloat16(1), jnp.bfloat16(0)).astype(HOT)


def is_end(line, lines):
    return line in (0, lines - 1)


def given(line, lines):
    outer = line - 1 if line < lines // 2 else line + 1
    return outer if not is_end(line, lines) and is_end(outer, lines) else None


def arrival_order(line, lines):
    stages = [(0, 1, 0, line)]
    for source in range(lines):
        gap = abs(source - line)
        if gap:
            split = is_end(line, lines) and gap > 1
            shared = given(line, lines) is not None and gap == 1 and source != given(line, lines)
            stages += [(gap - 1, 0, gap, source), (lines if split else 2 if shared else gap, 1, gap, source)]
    return sorted(stages)


def link_pieces(line, lines, pieces):
    def extra(to):
        if not 0 <= to < lines:
            return 0
        if is_end(to, lines):
            return lines - 2
        return 0 if given(to, lines) is None else pieces if given(to, lines) == line else pieces // 2

    up = pieces * (line + 1) + extra(line + 1) if line < lines - 1 else 0
    down = pieces * (lines - line) + extra(line - 1) if line > 0 else 0
    across = pieces * lines
    if given(line, lines) is not None:
        across -= pieces + pieces // 2
    if is_end(line, lines):
        across -= lines - 2
    return up, down, across


def return_order(line, lines):
    stages = [(0, 1, 0, line)]
    for source in range(lines):
        gap = abs(source - line)
        if gap:
            stages += [(gap - 1, 0, gap, source), (lines - 2 + gap, 1, gap, source)]
    return sorted(stages)


def return_pieces(line, lines, pieces):
    direct = lines > 2

    def one_way(to, behind, first):
        if not 0 <= to < lines:
            return 0
        onward = behind - (1 if direct and is_end(to, lines) and behind else 0)
        beside = pieces - EARLY if is_end(to, lines) else pieces if given(to, lines) == line else 0
        return pieces * (1 + (1 if direct and first else 0) + onward) + beside

    up = one_way(line + 1, line, line == 0)
    down = one_way(line - 1, lines - 1 - line, line == lines - 1)
    skipped = pieces if given(line, lines) is not None else pieces - EARLY if is_end(line, lines) else 0
    return up, down, pieces * lines - skipped


def graph_kernel(
    peers,
    x_ref, w_src_ref, bias_ref, embed_ref, w_node_ref, w_dec_ref, src_ref, dst_ref, count_ref,
    out_ref,
    x_all, idx_own, idx_in, src_vmem, dst_vmem, count_smem, w_src_all, bias_all, embed_all, w_node_all, w_dec_all,
    enc, dec, hot, msg, agg, acc, proj_mate, proj_all,
    ready, local_sem, par_send, par_recv, idx_send, idx_recv,
    x_send, xz_recv, xy_recv, xm_recv, p_send, pz_recv, py_recv, pm_recv, dec_send, dec_recv,
):
    lines = peers // 2
    me = lax.axis_index("graph")
    core = lax.axis_index("chan")
    mate = 1 - core
    line, side = me // 2, me % 2
    other = line * 2 + (1 - side)
    up, down = (line + 1) * 2 + side, (line - 1) * 2 + side
    has_up, has_down = line < lines - 1, line > 0
    low_half = line < lines // 2
    grid_rows, chans = x_ref.shape
    half_grid = grid_rows // 2
    block = half_grid // CHUNKS
    mesh_rows = embed_ref.shape[0]
    half_mesh = mesh_rows // 2
    part_mesh = half_mesh // SUBS
    cols = chans // 2
    capacity = src_ref.shape[2]
    UP, DOWN, ACROSS, MATE = range(4)

    def remote(src, dst, send, recv, graph, chan):
        return pltpu.make_async_remote_copy(
            src_ref=src, dst_ref=dst, send_sem=send, recv_sem=recv,
            device_id={"graph": graph, "chan": chan}, device_id_type=MESH,
        )

    def by_line(values):
        return sum(jnp.where(line == at, values[at], 0) for at in range(lines))

    end = (line == 0) | (line == lines - 1)
    giver = by_line([-1 if given(at, lines) is None else given(at, lines) for at in range(lines)])
    barrier = pltpu.get_barrier_semaphore()

    def greet(graph, chan):
        pl.semaphore_signal(barrier, inc=1, device_id={"graph": graph, "chan": chan}, device_id_type=MESH)

    greet(me, mate)
    for chan in (core, mate):
        greet(other, chan)
        pl.when(has_up)(functools.partial(greet, up, chan))
        pl.when(has_down)(functools.partial(greet, down, chan))
    my_rows = pl.ds(pl.multiple_of(core * half_mesh, half_mesh), half_mesh)
    mate_rows = pl.ds(pl.multiple_of(mate * half_mesh, half_mesh), half_mesh)
    own_rows = pl.ds(pl.multiple_of(me * grid_rows, grid_rows), grid_rows)
    locals_ = [
        pltpu.make_async_copy(src_ref, src_vmem, local_sem.at[0]),
        pltpu.make_async_copy(dst_ref, dst_vmem, local_sem.at[1]),
        pltpu.make_async_copy(count_ref, count_smem, local_sem.at[2]),
        pltpu.make_async_copy(x_ref, x_all.at[own_rows], local_sem.at[3]),
        pltpu.make_async_copy(w_src_ref, w_src_all.at[core], local_sem.at[4]),
        pltpu.make_async_copy(bias_ref, bias_all.at[core], local_sem.at[5]),
        pltpu.make_async_copy(w_node_ref, w_node_all.at[core], local_sem.at[6]),
        pltpu.make_async_copy(w_dec_ref, w_dec_all.at[core], local_sem.at[7]),
        pltpu.make_async_copy(embed_ref.at[my_rows], embed_all.at[core], local_sem.at[8]),
    ]
    for copy in locals_[3:4] + locals_[:3] + locals_[4:]:
        copy.start()
    locals_[3].wait()
    pl.semaphore_wait(barrier, 3 + 2 * jnp.where(has_up, 1, 0) + 2 * jnp.where(has_down, 1, 0))

    def x_part(shard, c, half=core):
        first = shard * grid_rows + c * 2 * block + half * block
        return x_all.at[pl.ds(pl.multiple_of(first, block), block)]

    def send_own(c):
        ref = x_part(me, c)
        for at, going, to, recv in (
            (UP, has_up, up, xz_recv), (DOWN, has_down, down, xz_recv), (ACROSS, None, other, xy_recv),
        ):
            def go(at=at, to=to, recv=recv):
                remote(ref, ref, x_send.at[at], recv.at[line, c], to, core).start()
            if going is None:
                go()
            else:
                pl.when(going)(go)

    send_own(0)
    for copy in locals_[:3]:
        copy.wait()
    slots = lax.broadcasted_iota(jnp.int32, (1, capacity), 1)
    for to in range(peers):
        idx_own[to, 0:1, :] = jnp.where(slots < count_smem[me, to], src_vmem[0, to : to + 1, :], -1)
        idx_own[to, 1:2, :] = dst_vmem[to]
    idx_in[me] = idx_own[me]

    def send_idx(to):
        remote(idx_own.at[to], idx_in.at[me], idx_send.at[0], idx_recv.at[me], to, core).start()

    send_idx(other)
    pl.when(has_up)(functools.partial(send_idx, up))
    pl.when(has_down)(functools.partial(send_idx, down))
    for c in range(1, CHUNKS - 1):
        send_own(c)
    for copy in locals_[4:]:
        copy.wait()
    par_copies = [
        remote(w_src_all.at[core], w_src_all.at[core], par_send.at[0], par_recv.at[0], me, mate),
        remote(bias_all.at[core], bias_all.at[core], par_send.at[1], par_recv.at[1], me, mate),
        remote(embed_ref.at[mate_rows], embed_all.at[core], par_send.at[2], par_recv.at[2], me, mate),
        remote(w_node_all.at[core], w_node_all.at[core], par_send.at[3], par_recv.at[3], me, mate),
        remote(w_dec_all.at[core], w_dec_all.at[core], par_send.at[4], par_recv.at[4], me, mate),
    ]
    for copy in par_copies:
        copy.start()

    def tell(at, to):
        pl.semaphore_signal(ready.at[at], inc=1, device_id={"graph": to, "chan": core}, device_id_type=MESH)

    pl.when(line == 0)(functools.partial(tell, 0, up))
    pl.when(line == lines - 1)(functools.partial(tell, 1, down))

    def relays(part, send, z_recv, y_recv, late, arrived, back=False):
        def extra(source, q, above):
            ref = part(source * 2 + 1 - side, q)
            remote(ref, ref, send.at[UP if above else DOWN], y_recv.at[source, q], up if above else down, core).start()

        def extras(source, q):
            for above, there in ((True, has_up), (False, has_down)):
                to = line + 1 if above else line - 1
                to_end = (to == 0) | (to == lines - 1)
                to_giver = by_line([
                    -1 if not 0 <= at + (1 if above else -1) < lines
                    or given(at + (1 if above else -1), lines) is None
                    else given(at + (1 if above else -1), lines)
                    for at in range(lines)
                ])
                wanted = (source == line) & (to_giver == line)
                if back:
                    wanted = (source == line) & ((to_giver == line) | to_end) if late(q) else wanted
                elif late(q):
                    wanted = wanted | (to_end & (jnp.abs(source - to) > 1))
                pl.when(there & wanted)(functools.partial(extra, source, q, above))

        def extras_inner(q):
            for above, there in ((True, has_up), (False, has_down)):
                step = 1 if above else -1
                wanted = by_line([
                    1 if 0 <= at + step < lines and given(at + step, lines) not in (None, at) else 0 for at in range(lines)
                ]) == 1
                pl.when(there & wanted)(functools.partial(extra, line, q, above))

        def take_line(i, q, which):
            for above in (True, False):
                source = line + 1 + i if above else line - 1 - i
                valid = (source < lines) if above else (source >= 0)
                if which is not None:
                    valid = valid & ((low_half if above else jnp.logical_not(low_half)) == (which == "inner"))
                onward, to, at = (has_down, down, DOWN) if above else (has_up, up, UP)

                @pl.when(valid)
                def _(source=source, onward=onward, to=to, at=at):
                    ref = part(source * 2 + side, q)
                    remote(ref, ref, send.at[at], z_recv.at[source, q], me, mate).wait_recv()

                    if back and lines > 2:
                        to_line = line - 1 if above else line + 1
                        onward = onward & ((to_line != (0 if above else lines - 1)) | (source != (lines - 1 if above else 0)))

                    @pl.when(onward)
                    def _():
                        remote(ref, ref, send.at[at], z_recv.at[source, q], to, core).start()

                    crossing = source != giver
                    if not back and q >= CHUNKS // 2:
                        crossing = crossing & ((giver < 0) | (jnp.abs(source - line) != 1))
                    if late(q):
                        gap_of = jnp.abs(source - line)
                        crossing = crossing & jnp.logical_not(end & ((gap_of == 1) if back else (gap_of > 1)))

                    @pl.when(crossing)
                    def _():
                        remote(ref, ref, send.at[ACROSS], y_recv.at[source, q], other, core).start()

                    arrived(source * 2 + side, q)

        def take_other(i, q):
            def take(source):
                shard = source * 2 + 1 - side
                ref = part(shard, q)
                remote(ref, ref, send.at[ACROSS], y_recv.at[source, q], me, mate).wait_recv()
                extras(source, q)
                arrived(shard, q)

            if i == 0:
                take(line)
                return
            for source, valid in ((line + i, line + i < lines), (line - i, line - i >= 0)):
                if late(q) and not back and i > 1:
                    valid = valid & jnp.logical_not(end)
                if not back and q >= CHUNKS // 2 and i == 1:
                    valid = valid & ((giver < 0) | (source == giver))
                pl.when(valid)(functools.partial(take, source))

        def take_far(i, q):
            pl.when(end)(functools.partial(take_one, jnp.where(low_half, line + i, line - i), q))

        def take_one(source, q, onward=False):
            shard = source * 2 + 1 - side
            ref = part(shard, q)
            remote(ref, ref, send.at[ACROSS], y_recv.at[source, q], me, mate).wait_recv()
            if onward:
                extras(source, q)
            arrived(shard, q)

        def take_shared(q):
            source = jnp.where(low_half, line + 1, line - 1)
            pl.when(giver >= 0)(functools.partial(take_one, source, q, onward=True))

        return take_line, take_other, take_far, extras_inner, take_shared

    def to_mate(shard, c):
        ref = x_part(shard, c)
        remote(ref, ref, x_send.at[MATE], xm_recv.at[shard, c // (CHUNKS // 2)], me, mate).start()

    nearest = [sorted((p for p in range(lines) if p != at), key=lambda p: (abs(p - at), p)) for at in range(lines)]
    sources = [by_line([nearest[at][i] for at in range(lines)]) for i in range(lines - 1)]
    build_order = [me, other]
    for i in range(lines):
        build_order += [source * 2 + side for source in sources[i : i + 1]]
        build_order += [source * 2 + 1 - side for source in sources[max(i - 1, 0) : i]]

    def by_stage(rule):
        tables = [rule(at, lines) for at in range(lines)]
        found = []
        for k in range(peers - 1):
            source = by_line([tables[at][k][3] for at in range(lines)])
            flip = by_line([tables[at][k][1] for at in range(lines)])
            stage = max(tables[at][k][0] for at in range(lines))
            found.append((stage, source * 2 + jnp.where(flip == 1, 1 - side, side)))
        return found

    order, order_back = by_stage(arrival_order), by_stage(return_order)

    def build_enc(shard, wait=True):
        if wait:
            remote(idx_own.at[0], idx_in.at[shard], idx_send.at[0], idx_recv.at[shard], me, mate).wait_recv()
        hot[:half_mesh, :] = one_hot(core * half_mesh, half_mesh, dst_vmem[shard])
        for t in range(2):
            picks = one_hot(t * half_grid, half_grid, idx_in[shard, 0:1, :])
            enc[shard, :, t * half_grid : (t + 1) * half_grid] = lax.dot_general(
                hot[:half_mesh, :], picks, NT, preferred_element_type=jnp.float32
            ).astype(jnp.bfloat16)

    pending = []

    def dec_copy(shard, half):
        ref = dec.at[shard, pl.ds(pl.multiple_of(half * half_grid, half_grid), half_grid)]
        return remote(ref, ref, dec_send.at[0], dec_recv.at[shard], me, mate)

    def flush():
        while pending:
            dec_copy(pending.pop(0), core).start()

    def build_dec(shard, wait=True):
        flush()
        hot[...] = one_hot(0, mesh_rows, idx_in[shard, 1:2, :])
        for t in range(half_grid // 256):
            first = pl.multiple_of(core * half_grid, half_grid) + t * 256
            picks = one_hot(first, 256, idx_own[shard, 0:1, :])
            dec[shard, pl.ds(pl.multiple_of(first, 256), 256), :] = lax.dot_general(
                picks, hot[...], NT, preferred_element_type=jnp.float32
            ).astype(jnp.bfloat16)
        pending.append(shard)

    def encode(shard, first=False, parts=(0, 1)):
        if not first:
            for part in parts:
                some = x_all.at[pl.ds(0, half_grid // 2)]
                remote(some, some, x_send.at[MATE], xm_recv.at[shard, part], me, mate).wait_recv()
        low, high = min(parts) * CHUNKS // 2, (max(parts) + 1) * CHUNKS // 2
        for c in range(low, high):
            rows = pl.ds(pl.multiple_of(shard * grid_rows, grid_rows) + c * 2 * block, 2 * block)
            for h in range(2):
                pre = jnp.dot(x_all[rows, :], w_src_all[h], preferred_element_type=jnp.float32) + bias_all[h]
                msg[c * 2 * block : (c + 1) * 2 * block, h * (msg.shape[1] // 2) : (h + 1) * (msg.shape[1] // 2)] = (
                    pre + pre * jnp.tanh(pre)
                ).astype(jnp.bfloat16)
        some = slice(low * 2 * block, high * 2 * block)
        total = jnp.dot(enc[shard, :, some], msg[some, :], preferred_element_type=jnp.float32)
        if first:
            agg[...] = total
        else:
            agg[...] += total

    def poll(hop):
        @pl.when(line == hop + 1)
        def _():
            pl.semaphore_wait(ready.at[0], 1)
            pl.when(has_up)(functools.partial(tell, 0, up))

        @pl.when(line == lines - 2 - hop)
        def _():
            pl.semaphore_wait(ready.at[1], 1)
            pl.when(has_down)(functools.partial(tell, 1, down))

        known = by_line([max(at - 1, lines - 2 - at) for at in range(lines)]) == hop
        for source in range(lines):
            for its_side in range(2):
                near = jnp.where(side == its_side, jnp.abs(line - source), 2 * jnp.abs(line - source) + 1) <= 1
                pl.when(known & jnp.logical_not(near))(functools.partial(send_idx, source * 2 + its_side))

    poll(0)
    build_enc(me, wait=False)
    build_dec(me, wait=False)
    for copy in par_copies:
        copy.wait()
    w_src_all[...] = w_src_all[...] * 0.5
    bias_all[...] = bias_all[...] * 0.5
    encode(me, first=True)
    poll(1)
    send_own(CHUNKS - 1)
    enc_tasks = [functools.partial(build_enc, shard) for shard in build_order[1:]]
    dec_tasks = [functools.partial(build_dec, shard, wait=False) for shard in build_order[1:]]
    tasks = [task for pair in zip(enc_tasks[:-2], dec_tasks[:-2]) for task in pair] + enc_tasks[-2:]
    dec_tasks = dec_tasks[-2:]

    def run(count):
        for _ in range(min(count, len(tasks))):
            tasks.pop(0)()

    def halves(c):
        return c == CHUNKS - 1

    take_line, take_other, take_far, extras_inner, take_shared = relays(x_part, x_send, xz_recv, xy_recv, halves, to_mate)
    def encodes(stage, parts):
        return [functools.partial(encode, shard, parts=parts) for at, shard in order if at == stage]

    run(2)
    for hop in range(2, lines - 1):
        poll(hop)
    for i in range(lines - 1):
        for c in range(CHUNKS):
            take_line(i, c, None)
            take_other(i, c)
            if i == 2 and c < CHUNKS // 2:
                take_shared(CHUNKS // 2 + c)
            if i == lines - 2 and c == CHUNKS // 2:
                tasks += encodes(i, (0,))
            run(1 + c // 2 if i == 0 else -(-len(tasks) // (CHUNKS - c)))
        if i == 0 and lines > 2:
            for c in range(CHUNKS // 2, CHUNKS):
                extras_inner(c)
        tasks += encodes(i, (0, 1) if i < lines - 2 else (1,))
    tasks += encodes(lines, (0,))
    for c in range(CHUNKS - 1):
        take_other(lines - 1, c)
        if c == CHUNKS - 2:
            for gap in range(2, lines - 1):
                take_far(gap, CHUNKS - 1)
        run(-(-len(tasks) // (CHUNKS - 1 - c)))
    if lines > 2:
        take_far(lines - 1, CHUNKS - 1)
    for task in encodes(lines, (1,)):
        task()

    width = agg.shape[1] // 2
    my_first = pl.multiple_of(me * mesh_rows + core * half_mesh, half_mesh)

    def p_part(shard, q):
        flip, sub = q % 2, q // 2
        half = mate if flip else core
        first = shard * mesh_rows + half * half_mesh + sub * part_mesh
        return proj_all.at[pl.ds(pl.multiple_of(first, part_mesh), part_mesh)]

    for sub in range(SUBS):
        some = slice(sub * part_mesh, (sub + 1) * part_mesh)
        hidden = sum(
            jnp.dot(
                agg[some, h * width : (h + 1) * width].astype(jnp.bfloat16), w_node_all[h],
                preferred_element_type=jnp.float32,
            )
            for h in range(2)
        )
        projected = sum(
            jnp.dot(
                (
                    embed_all[h, some, :].astype(jnp.float32) + silu(hidden[:, h * width : (h + 1) * width])
                ).astype(jnp.bfloat16),
                w_dec_all[h], preferred_element_type=jnp.float32,
            )
            for h in range(2)
        ).astype(jnp.bfloat16)
        first_core = core == 0
        into = p_part(me, 2 * sub)
        proj_all[pl.ds(pl.multiple_of(my_first + sub * part_mesh, part_mesh), part_mesh), :] = jnp.where(
            first_core, projected[:, :cols], projected[:, cols:]
        )
        proj_mate[some, :] = jnp.where(first_core, projected[:, cols:], projected[:, :cols])
        for flip in range(2):
            ref = proj_mate.at[pl.ds(sub * part_mesh, part_mesh)] if flip else into
            chan = mate if flip else core
            routes = [(UP, has_up, up, pz_recv), (DOWN, has_down, down, pz_recv), (ACROSS, None, other, py_recv)]
            if lines > 2:
                routes[:0] = [
                    (UP, line == 0, (lines - 1) * 2 + side, pz_recv), (DOWN, line == lines - 1, side, pz_recv),
                ]
            for at, going, to, recv in routes:
                def go(ref=ref, into=into, at=at, to=to, recv=recv, q=2 * sub + flip, chan=chan):
                    remote(ref, into, p_send.at[at], recv.at[line, q], to, chan).start()
                if going is None:
                    go()
                else:
                    pl.when(going)(go)
    whole_half = proj_all.at[pl.ds(my_first, half_mesh)]
    remote(proj_mate, whole_half, p_send.at[MATE], pm_recv.at[0], me, mate).start()

    def decode(*shards):
        some = dec.at[0, pl.ds(0, half_grid)]
        for shard in shards:
            remote(some, some, dec_send.at[0], dec_recv.at[shard], me, mate).wait_recv()
        for t in range(2):
            at = pl.ds(t * half_grid, half_grid)
            acc[at, :] += sum(
                jnp.dot(
                    dec[shard, at, :], proj_all[pl.ds(pl.multiple_of(shard * mesh_rows, mesh_rows), mesh_rows), :],
                    preferred_element_type=jnp.float32,
                )
                for shard in shards
            )

    take_line, take_other, *_ = relays(
        p_part, p_send, pz_recv, py_recv, lambda q: q >= EARLY, lambda shard, q: None, back=True)
    acc[...] = x_all[own_rows, pl.ds(pl.multiple_of(core * cols, cols), cols)].astype(jnp.float32)

    def own_decode():
        remote(proj_mate, whole_half, p_send.at[MATE], pm_recv.at[0], me, mate).wait_recv()
        decode(me)

    pieces = 2 * SUBS
    tasks += dec_tasks
    run(len(tasks))
    flush()
    tasks.append(own_decode)

    for q in range(pieces):
        take_line(0, q, "inner")
        if q:
            take_other(0, q - 1)
    take_other(0, pieces - 1)
    for q in range(pieces):
        take_line(0, q, "outer")
    for q in range(pieces):
        for i in range(1, lines - 1):
            take_line(i, q, "inner")
            take_line(i, q, "outer")
        if q % 2:
            run(1)
    run(len(tasks))
    early = [shard for at, shard in order_back if at < lines - 1]
    for n in range(0, len(early), 2):
        decode(*early[n : n + 2])
    for q in range(pieces):
        for i in range(1, lines):
            if i > 1 or q < EARLY:
                take_other(i, q)
        if q == pieces - 2:
            for late_q in range(EARLY, pieces):
                take_other(1, late_q)
            for at, shard in order_back:
                if at == lines - 1:
                    decode(shard)
    final = [shard for at, shard in order_back if at >= lines]
    if final:
        decode(*final)
    out_ref[...] = acc[...].astype(jnp.bfloat16)

    def drained(ref, sem):
        remote(ref, ref, sem, sem, me, mate).wait_send()

    for at in range(lines):
        @pl.when(line == at)
        def _(at=at):
            for n, (x_n, p_n) in enumerate(zip(link_pieces(at, lines, CHUNKS), return_pieces(at, lines, pieces))):
                if x_n:
                    drained(x_all.at[pl.ds(0, x_n * block)], x_send.at[n])
                    drained(proj_all.at[pl.ds(0, p_n * part_mesh)], p_send.at[n])
    drained(x_all.at[pl.ds(0, (peers - 1) * half_grid)], x_send.at[MATE])
    drained(proj_mate, p_send.at[MATE])
    drained(idx_own.at[pl.ds(0, peers - 1)], idx_send.at[0])
    drained(dec.at[:, pl.ds(0, half_grid)], dec_send.at[0])


def fused(grid_state, w_src, bias_src, mesh_embed, w_node, w_dec, slot_src, slot_dst, slot_count):
    peers = lax.axis_size("graph")
    capacity = slot_src.shape[2]
    grid_rows, chans = grid_state.shape
    mesh_rows = mesh_embed.shape[0]
    hidden = w_src.shape[1]
    lines = peers // 2
    bf16, f32, i32 = jnp.bfloat16, jnp.float32, jnp.int32
    dma = pltpu.SemaphoreType.DMA
    pieces = 2 * SUBS
    return pl.pallas_call(
        functools.partial(graph_kernel, peers),
        out_shape=jax.ShapeDtypeStruct((grid_rows, chans // 2), bf16),
        in_specs=[pl.BlockSpec(memory_space=pl.ANY)] * 9,
        out_specs=pl.BlockSpec(memory_space=pltpu.VMEM),
        scratch_shapes=[
            pltpu.VMEM((peers * grid_rows, chans), bf16),
            pltpu.VMEM((peers, 2, capacity), i32),
            pltpu.VMEM((peers, 2, capacity), i32),
            pltpu.VMEM(slot_src.shape, i32),
            pltpu.VMEM(slot_dst.shape, i32),
            pltpu.SMEM(slot_count.shape, i32),
            pltpu.VMEM((2,) + w_src.shape, bf16),
            pltpu.VMEM((2, 1, hidden), f32),
            pltpu.VMEM((2, mesh_rows // 2, hidden), bf16),
            pltpu.VMEM((2,) + w_node.shape, bf16),
            pltpu.VMEM((2,) + w_dec.shape, bf16),
            pltpu.VMEM((peers, mesh_rows // 2, grid_rows), bf16),
            pltpu.VMEM((peers, grid_rows, mesh_rows), bf16),
            pltpu.VMEM((mesh_rows, capacity), HOT),
            pltpu.VMEM((grid_rows, 2 * hidden), bf16),
            pltpu.VMEM((mesh_rows // 2, 2 * hidden), f32),
            pltpu.VMEM((grid_rows, chans // 2), f32),
            pltpu.VMEM((mesh_rows // 2, chans // 2), bf16),
            pltpu.VMEM((peers * mesh_rows, chans // 2), bf16),
            pltpu.SemaphoreType.REGULAR((2,)),
            dma((9,)), dma((5,)), dma((5,)), dma((1,)), dma((peers,)),
            dma((4,)), dma((lines, CHUNKS)), dma((lines, CHUNKS)), dma((peers, 2)),
            dma((4,)), dma((lines, pieces)), dma((lines, pieces)), dma((1,)), dma((1,)), dma((peers,)),
        ],
        compiler_params=pltpu.CompilerParams(collective_id=0, has_side_effects=True),
    )(grid_state, w_src, bias_src[None, :], mesh_embed, w_node, w_dec, slot_src, slot_dst, slot_count)


def held_bytes(peers, grid_state, mesh_embed, *rest):
    grid_rows, chans = grid_state.shape
    mesh_rows = mesh_embed.shape[0]
    return 2 * peers * grid_rows * (chans + 2 * mesh_rows)


def per_device(grid_state, w_src, bias_src, mesh_embed, *rest):
    peers = lax.axis_size("graph")
    fits = (
        peers % 2 == 0
        and peers in (4, 8)
        and lax.axis_size("chan") == 2
        and held_bytes(peers, grid_state, mesh_embed) <= VMEM_BUDGET
    )
    body = fused if fits else on_device
    return body(grid_state, w_src, bias_src, mesh_embed, *rest)


def solution(mesh):
    placed = (
        P(("member", "graph"), None),
        P(None, "chan"),
        P("chan"),
        P("graph", "chan"),
        P("chan", None),
        P("chan", None),
        P("graph", None, None),
        P(None, "graph", None),
        P(),
    )
    return jax.shard_map(
        per_device,
        mesh=mesh,
        in_specs=placed,
        out_specs=P(("member", "graph"), "chan"),
        check_vma=False,
    )
```

```python
import functools
import math

import jax
import jax.numpy as jnp
from jax import lax
from jax.experimental import pallas as pl
from jax.experimental.pallas import tpu as pltpu
from jax.sharding import PartitionSpec as P

CHUNKS = 4
SUBS = 2
EARLY = 1
HOT = jnp.float8_e4m3fn
VMEM_BUDGET = 48 * 2**20
MESH = pl.DeviceIdType.MESH
NT = (((1,), (1,)), ((), ()))


def edge_network(source_rows, w_src, bias_src):
    return jax.nn.silu(
        jnp.dot(source_rows, w_src, preferred_element_type=jnp.float32) + bias_src
    ).astype(jnp.bfloat16)


def segment_rows(values, indices, usable, row_count):
    slot_total = values.shape[0]
    width = values.shape[1]
    block_len = math.gcd(slot_total, 2048)
    block_count = slot_total // block_len
    targets = jnp.where(usable, indices, -1).reshape(block_count, block_len)
    pieces = values.reshape(block_count, block_len, width)
    row_ids = jnp.arange(row_count, dtype=jnp.int32)

    def add_block(summed, scan_item):
        row_target, piece_vals = scan_item
        one_hot = (row_ids[:, None] == row_target[None, :]).astype(jnp.bfloat16)
        return (summed + jnp.dot(one_hot, piece_vals, preferred_element_type=jnp.float32), None)

    result, unused = lax.scan(
        add_block, jnp.zeros((row_count, width), jnp.float32), (targets, pieces)
    )
    return result


def on_device(
    grid_state, w_src, bias_src, mesh_embed, w_node, w_dec, slot_src, slot_dst, slot_count
):
    peers = lax.axis_size("graph")
    own_index = lax.axis_index("graph")
    core_index = lax.axis_index("chan")
    capacity = slot_src.shape[2]
    positions = jnp.arange(capacity, dtype=jnp.int32)
    grid_rows = grid_state.shape[0]
    mesh_rows = mesh_embed.shape[0]
    sent_counts = lax.dynamic_slice_in_dim(slot_count, own_index, 1, 0)[0]
    recv_counts = lax.dynamic_slice_in_dim(slot_count, own_index, 1, 1)[:, 0]
    half_slots = capacity // 2
    chosen = lax.dynamic_slice_in_dim(slot_src[0], core_index * half_slots, half_slots, 1)
    picked = jnp.take(grid_state, chosen.reshape(-1), axis=0).reshape(
        peers, half_slots, grid_state.shape[1]
    )
    arrived = lax.all_to_all(picked, "graph", split_axis=0, concat_axis=0, tiled=True)
    joined = lax.all_gather(arrived, "chan", axis=1, tiled=True)
    messages = edge_network(joined.reshape(peers * capacity, grid_state.shape[1]), w_src, bias_src)
    arrive_ok = (positions[None, :] < recv_counts[:, None]).reshape(-1)
    dst_rows = slot_dst[:, 0, :].reshape(-1)
    aggregate = segment_rows(messages, dst_rows, arrive_ok, mesh_rows)
    partial_hidden = jnp.dot(
        aggregate.astype(jnp.bfloat16), w_node, preferred_element_type=jnp.float32
    )
    hidden_pre = lax.psum_scatter(partial_hidden, "chan", scatter_dimension=1, tiled=True)
    latent = (mesh_embed.astype(jnp.float32) + jax.nn.silu(hidden_pre)).astype(jnp.bfloat16)
    partial_proj = jnp.dot(latent, w_dec, preferred_element_type=jnp.float32)
    projected = lax.psum_scatter(partial_proj, "chan", scatter_dimension=1, tiled=True).astype(
        jnp.bfloat16
    )
    returned = jnp.take(projected, dst_rows, axis=0).reshape(peers, capacity, projected.shape[1])
    came_back = lax.all_to_all(returned, "graph", split_axis=0, concat_axis=0, tiled=True).reshape(
        peers * capacity, projected.shape[1]
    )
    send_ok = (positions[None, :] < sent_counts[:, None]).reshape(-1)
    decoded = segment_rows(came_back, slot_src[0].reshape(-1), send_ok, grid_rows)
    width_half = decoded.shape[1]
    own_cols = lax.dynamic_slice_in_dim(grid_state, core_index * width_half, width_half, 1)
    return (own_cols.astype(jnp.float32) + decoded).astype(jnp.bfloat16)


def silu(v):
    half = 0.5 * v
    return half + half * jnp.tanh(half)


def one_hot(first, rows, indices):
    row_ids = lax.broadcasted_iota(jnp.int16, (rows, indices.shape[1]), 0)
    hits = row_ids == (indices - first).astype(jnp.int16)
    return jnp.where(hits, jnp.bfloat16(1), jnp.bfloat16(0)).astype(HOT)


def is_end(line, lines):
    return line in (0, lines - 1)


def given(line, lines):
    outer = line - 1 if line < lines // 2 else line + 1
    return outer if not is_end(line, lines) and is_end(outer, lines) else None


def arrival_order(line, lines):
    stages = [(0, 1, 0, line)]
    for source in range(lines):
        gap = abs(source - line)
        if gap:
            split = is_end(line, lines) and gap > 1
            shared = given(line, lines) is not None and gap == 1 and source != given(line, lines)
            stages += [(gap - 1, 0, gap, source), (lines if split else 2 if shared else gap, 1, gap, source)]
    return sorted(stages)


def link_pieces(line, lines, pieces):
    def extra(to):
        if not 0 <= to < lines:
            return 0
        if is_end(to, lines):
            return lines - 2
        return 0 if given(to, lines) is None else pieces if given(to, lines) == line else pieces // 2

    up = pieces * (line + 1) + extra(line + 1) if line < lines - 1 else 0
    down = pieces * (lines - line) + extra(line - 1) if line > 0 else 0
    across = pieces * lines
    if given(line, lines) is not None:
        across -= pieces + pieces // 2
    if is_end(line, lines):
        across -= lines - 2
    return up, down, across


def return_order(line, lines):
    stages = [(0, 1, 0, line)]
    for source in range(lines):
        gap = abs(source - line)
        if gap:
            stages += [(gap - 1, 0, gap, source), (lines - 2 + gap, 1, gap, source)]
    return sorted(stages)


def return_pieces(line, lines, pieces):
    direct = lines > 2

    def one_way(to, behind, first):
        if not 0 <= to < lines:
            return 0
        onward = behind - (1 if direct and is_end(to, lines) and behind else 0)
        beside = pieces - EARLY if direct and is_end(to, lines) else pieces if given(to, lines) == line else 0
        return pieces * (1 + (1 if direct and first else 0) + onward) + beside

    up = one_way(line + 1, line, line == 0)
    down = one_way(line - 1, lines - 1 - line, line == lines - 1)
    skipped = pieces if given(line, lines) is not None else pieces - EARLY if lines > 2 and is_end(line, lines) else 0
    return up, down, pieces * lines - skipped


def graph_kernel(
    peers,
    x_ref, w_src_ref, bias_ref, embed_ref, w_node_ref, w_dec_ref, src_ref, dst_ref, count_ref,
    out_ref,
    x_all, idx_own, idx_in, src_vmem, dst_vmem, count_smem, w_src_all, bias_all, embed_all, w_node_all, w_dec_all,
    enc, dec, hot, msg, agg, acc, proj_mate, proj_all,
    ready, local_sem, par_send, par_recv, idx_send, idx_recv,
    x_send, xz_recv, xy_recv, xm_recv, p_send, pz_recv, py_recv, pm_recv, dec_send, dec_recv,
):
    lines = peers // 2
    me = lax.axis_index("graph")
    core = lax.axis_index("chan")
    mate = 1 - core
    line, side = me // 2, me % 2
    other = line * 2 + (1 - side)
    up, down = (line + 1) * 2 + side, (line - 1) * 2 + side
    has_up, has_down = line < lines - 1, line > 0
    low_half = line < lines // 2
    grid_rows, chans = x_ref.shape
    half_grid = grid_rows // 2
    block = half_grid // CHUNKS
    mesh_rows = embed_ref.shape[0]
    half_mesh = mesh_rows // 2
    part_mesh = half_mesh // SUBS
    cols = chans // 2
    capacity = src_ref.shape[2]
    UP, DOWN, ACROSS, MATE = range(4)

    def remote(src, dst, send, recv, graph, chan):
        return pltpu.make_async_remote_copy(
            src_ref=src, dst_ref=dst, send_sem=send, recv_sem=recv,
            device_id={"graph": graph, "chan": chan}, device_id_type=MESH,
        )

    def by_line(values):
        return sum(jnp.where(line == at, values[at], 0) for at in range(lines))

    end = (line == 0) | (line == lines - 1)
    giver = by_line([-1 if given(at, lines) is None else given(at, lines) for at in range(lines)])
    barrier = pltpu.get_barrier_semaphore()

    def greet(graph, chan):
        pl.semaphore_signal(barrier, inc=1, device_id={"graph": graph, "chan": chan}, device_id_type=MESH)

    greet(me, mate)
    for chan in (core, mate):
        greet(other, chan)
        pl.when(has_up)(functools.partial(greet, up, chan))
        pl.when(has_down)(functools.partial(greet, down, chan))
    my_rows = pl.ds(pl.multiple_of(core * half_mesh, half_mesh), half_mesh)
    mate_rows = pl.ds(pl.multiple_of(mate * half_mesh, half_mesh), half_mesh)
    own_rows = pl.ds(pl.multiple_of(me * grid_rows, grid_rows), grid_rows)
    locals_ = [
        pltpu.make_async_copy(src_ref, src_vmem, local_sem.at[0]),
        pltpu.make_async_copy(dst_ref, dst_vmem, local_sem.at[1]),
        pltpu.make_async_copy(count_ref, count_smem, local_sem.at[2]),
        pltpu.make_async_copy(x_ref, x_all.at[own_rows], local_sem.at[3]),
        pltpu.make_async_copy(w_src_ref, w_src_all.at[core], local_sem.at[4]),
        pltpu.make_async_copy(bias_ref, bias_all.at[core], local_sem.at[5]),
        pltpu.make_async_copy(w_node_ref, w_node_all.at[core], local_sem.at[6]),
        pltpu.make_async_copy(w_dec_ref, w_dec_all.at[core], local_sem.at[7]),
        pltpu.make_async_copy(embed_ref.at[my_rows], embed_all.at[core], local_sem.at[8]),
    ]
    for copy in locals_[3:4] + locals_[:3] + locals_[4:]:
        copy.start()
    locals_[3].wait()
    pl.semaphore_wait(barrier, 3 + 2 * jnp.where(has_up, 1, 0) + 2 * jnp.where(has_down, 1, 0))

    def x_part(shard, c, half=core):
        first = shard * grid_rows + c * 2 * block + half * block
        return x_all.at[pl.ds(pl.multiple_of(first, block), block)]

    def send_own(c):
        ref = x_part(me, c)
        for at, going, to, recv in (
            (UP, has_up, up, xz_recv), (DOWN, has_down, down, xz_recv), (ACROSS, None, other, xy_recv),
        ):
            def go(at=at, to=to, recv=recv):
                remote(ref, ref, x_send.at[at], recv.at[line, c], to, core).start()
            if going is None:
                go()
            else:
                pl.when(going)(go)

    send_own(0)
    for copy in locals_[:3]:
        copy.wait()
    slots = lax.broadcasted_iota(jnp.int32, (1, capacity), 1)
    for to in range(peers):
        idx_own[to, 0:1, :] = jnp.where(slots < count_smem[me, to], src_vmem[0, to : to + 1, :], -1)
        idx_own[to, 1:2, :] = dst_vmem[to]
    idx_in[me] = idx_own[me]

    def send_idx(to):
        remote(idx_own.at[to], idx_in.at[me], idx_send.at[0], idx_recv.at[me], to, core).start()

    send_idx(other)
    pl.when(has_up)(functools.partial(send_idx, up))
    pl.when(has_down)(functools.partial(send_idx, down))
    for c in range(1, CHUNKS - 1):
        send_own(c)
    for copy in locals_[4:]:
        copy.wait()
    par_copies = [
        remote(w_src_all.at[core], w_src_all.at[core], par_send.at[0], par_recv.at[0], me, mate),
        remote(bias_all.at[core], bias_all.at[core], par_send.at[1], par_recv.at[1], me, mate),
        remote(embed_ref.at[mate_rows], embed_all.at[core], par_send.at[2], par_recv.at[2], me, mate),
        remote(w_node_all.at[core], w_node_all.at[core], par_send.at[3], par_recv.at[3], me, mate),
        remote(w_dec_all.at[core], w_dec_all.at[core], par_send.at[4], par_recv.at[4], me, mate),
    ]
    for copy in par_copies:
        copy.start()

    def tell(at, to):
        pl.semaphore_signal(ready.at[at], inc=1, device_id={"graph": to, "chan": core}, device_id_type=MESH)

    pl.when(line == 0)(functools.partial(tell, 0, up))
    pl.when(line == lines - 1)(functools.partial(tell, 1, down))

    def relays(part, send, z_recv, y_recv, late, arrived, back=False):
        def extra(source, q, above):
            ref = part(source * 2 + 1 - side, q)
            remote(ref, ref, send.at[UP if above else DOWN], y_recv.at[source, q], up if above else down, core).start()

        def extras(source, q):
            for above, there in ((True, has_up), (False, has_down)):
                to = line + 1 if above else line - 1
                to_end = (to == 0) | (to == lines - 1)
                to_giver = by_line([
                    -1 if not 0 <= at + (1 if above else -1) < lines
                    or given(at + (1 if above else -1), lines) is None
                    else given(at + (1 if above else -1), lines)
                    for at in range(lines)
                ])
                wanted = (source == line) & (to_giver == line)
                if late(q):
                    gap_to = jnp.abs(source - to)
                    wanted = wanted | (to_end & ((gap_to == 2) if back else (gap_to > 1)))
                pl.when(there & wanted)(functools.partial(extra, source, q, above))

        def extras_inner(q):
            for above, there in ((True, has_up), (False, has_down)):
                step = 1 if above else -1
                wanted = by_line([
                    1 if 0 <= at + step < lines and given(at + step, lines) not in (None, at) else 0 for at in range(lines)
                ]) == 1
                pl.when(there & wanted)(functools.partial(extra, line, q, above))

        def take_line(i, q, which):
            for above in (True, False):
                source = line + 1 + i if above else line - 1 - i
                valid = (source < lines) if above else (source >= 0)
                if which is not None:
                    valid = valid & ((low_half if above else jnp.logical_not(low_half)) == (which == "inner"))
                onward, to, at = (has_down, down, DOWN) if above else (has_up, up, UP)

                @pl.when(valid)
                def _(source=source, onward=onward, to=to, at=at):
                    ref = part(source * 2 + side, q)
                    remote(ref, ref, send.at[at], z_recv.at[source, q], me, mate).wait_recv()

                    if back and lines > 2:
                        to_line = line - 1 if above else line + 1
                        onward = onward & ((to_line != (0 if above else lines - 1)) | (source != (lines - 1 if above else 0)))

                    @pl.when(onward)
                    def _():
                        remote(ref, ref, send.at[at], z_recv.at[source, q], to, core).start()

                    crossing = source != giver
                    if not back and q >= CHUNKS // 2:
                        crossing = crossing & ((giver < 0) | (jnp.abs(source - line) != 1))
                    if late(q):
                        gap_of = jnp.abs(source - line)
                        crossing = crossing & jnp.logical_not(end & ((gap_of == 2) if back else (gap_of > 1)))

                    @pl.when(crossing)
                    def _():
                        remote(ref, ref, send.at[ACROSS], y_recv.at[source, q], other, core).start()

                    arrived(source * 2 + side, q)

        def take_other(i, q):
            def take(source):
                shard = source * 2 + 1 - side
                ref = part(shard, q)
                remote(ref, ref, send.at[ACROSS], y_recv.at[source, q], me, mate).wait_recv()
                extras(source, q)
                arrived(shard, q)

            if i == 0:
                take(line)
                return
            for source, valid in ((line + i, line + i < lines), (line - i, line - i >= 0)):
                if late(q) and not back and i > 1:
                    valid = valid & jnp.logical_not(end)
                if i == 1 and (back or q >= CHUNKS // 2):
                    valid = valid & ((giver < 0) | (source == giver))
                pl.when(valid)(functools.partial(take, source))

        def take_far(i, q):
            pl.when(end)(functools.partial(take_one, jnp.where(low_half, line + i, line - i), q))

        def take_one(source, q, onward=False):
            shard = source * 2 + 1 - side
            ref = part(shard, q)
            remote(ref, ref, send.at[ACROSS], y_recv.at[source, q], me, mate).wait_recv()
            if onward:
                extras(source, q)
            arrived(shard, q)

        def take_shared(q):
            source = jnp.where(low_half, line + 1, line - 1)
            pl.when(giver >= 0)(functools.partial(take_one, source, q, onward=True))

        return take_line, take_other, take_far, extras_inner, take_shared

    def to_mate(shard, c):
        ref = x_part(shard, c)
        remote(ref, ref, x_send.at[MATE], xm_recv.at[shard, c // (CHUNKS // 2)], me, mate).start()

    nearest = [sorted((p for p in range(lines) if p != at), key=lambda p: (abs(p - at), p)) for at in range(lines)]
    sources = [by_line([nearest[at][i] for at in range(lines)]) for i in range(lines - 1)]
    build_order = [me, other]
    for i in range(lines):
        build_order += [source * 2 + side for source in sources[i : i + 1]]
        build_order += [source * 2 + 1 - side for source in sources[max(i - 1, 0) : i]]

    def by_stage(rule):
        tables = [rule(at, lines) for at in range(lines)]
        found = []
        for k in range(peers - 1):
            source = by_line([tables[at][k][3] for at in range(lines)])
            flip = by_line([tables[at][k][1] for at in range(lines)])
            stage = max(tables[at][k][0] for at in range(lines))
            found.append((stage, source * 2 + jnp.where(flip == 1, 1 - side, side)))
        return found

    order, order_back = by_stage(arrival_order), by_stage(return_order)

    def build_enc(shard, wait=True):
        if wait:
            remote(idx_own.at[0], idx_in.at[shard], idx_send.at[0], idx_recv.at[shard], me, mate).wait_recv()
        hot[:half_mesh, :] = one_hot(core * half_mesh, half_mesh, dst_vmem[shard])
        for t in range(2):
            picks = one_hot(t * half_grid, half_grid, idx_in[shard, 0:1, :])
            enc[shard, :, t * half_grid : (t + 1) * half_grid] = lax.dot_general(
                hot[:half_mesh, :], picks, NT, preferred_element_type=jnp.float32
            ).astype(jnp.bfloat16)

    pending = []

    def dec_copy(shard, half):
        ref = dec.at[shard, pl.ds(pl.multiple_of(half * half_grid, half_grid), half_grid)]
        return remote(ref, ref, dec_send.at[0], dec_recv.at[shard], me, mate)

    def flush():
        while pending:
            dec_copy(pending.pop(0), core).start()

    def build_dec(shard, wait=True):
        flush()
        hot[...] = one_hot(0, mesh_rows, idx_in[shard, 1:2, :])
        for t in range(half_grid // 256):
            first = pl.multiple_of(core * half_grid, half_grid) + t * 256
            picks = one_hot(first, 256, idx_own[shard, 0:1, :])
            dec[shard, pl.ds(pl.multiple_of(first, 256), 256), :] = lax.dot_general(
                picks, hot[...], NT, preferred_element_type=jnp.float32
            ).astype(jnp.bfloat16)
        pending.append(shard)

    def encode(shard, first=False, parts=(0, 1)):
        if not first:
            for part in parts:
                some = x_all.at[pl.ds(0, half_grid // 2)]
                remote(some, some, x_send.at[MATE], xm_recv.at[shard, part], me, mate).wait_recv()
        low, high = min(parts) * CHUNKS // 2, (max(parts) + 1) * CHUNKS // 2
        for c in range(low, high):
            rows = pl.ds(pl.multiple_of(shard * grid_rows, grid_rows) + c * 2 * block, 2 * block)
            for h in range(2):
                pre = jnp.dot(x_all[rows, :], w_src_all[h], preferred_element_type=jnp.float32) + bias_all[h]
                msg[c * 2 * block : (c + 1) * 2 * block, h * (msg.shape[1] // 2) : (h + 1) * (msg.shape[1] // 2)] = (
                    pre + pre * jnp.tanh(pre)
                ).astype(jnp.bfloat16)
        some = slice(low * 2 * block, high * 2 * block)
        total = jnp.dot(enc[shard, :, some], msg[some, :], preferred_element_type=jnp.float32)
        if first:
            agg[...] = total
        else:
            agg[...] += total

    def poll(hop):
        @pl.when(line == hop + 1)
        def _():
            pl.semaphore_wait(ready.at[0], 1)
            pl.when(has_up)(functools.partial(tell, 0, up))

        @pl.when(line == lines - 2 - hop)
        def _():
            pl.semaphore_wait(ready.at[1], 1)
            pl.when(has_down)(functools.partial(tell, 1, down))

        known = by_line([max(at - 1, lines - 2 - at) for at in range(lines)]) == hop
        for source in range(lines):
            for its_side in range(2):
                near = jnp.where(side == its_side, jnp.abs(line - source), 2 * jnp.abs(line - source) + 1) <= 1
                pl.when(known & jnp.logical_not(near))(functools.partial(send_idx, source * 2 + its_side))

    poll(0)
    build_enc(me, wait=False)
    build_dec(me, wait=False)
    for copy in par_copies:
        copy.wait()
    w_src_all[...] = w_src_all[...] * 0.5
    bias_all[...] = bias_all[...] * 0.5
    encode(me, first=True)
    poll(1)
    send_own(CHUNKS - 1)
    enc_tasks = [functools.partial(build_enc, shard) for shard in build_order[1:]]
    dec_tasks = [functools.partial(build_dec, shard, wait=False) for shard in build_order[1:]]
    tasks = [task for pair in zip(enc_tasks[:-2], dec_tasks[:-2]) for task in pair] + enc_tasks[-2:]
    dec_tasks = dec_tasks[-2:]

    def run(count):
        for _ in range(min(count, len(tasks))):
            tasks.pop(0)()

    def halves(c):
        return c == CHUNKS - 1

    take_line, take_other, take_far, extras_inner, take_shared = relays(x_part, x_send, xz_recv, xy_recv, halves, to_mate)
    def encodes(stage, parts):
        return [functools.partial(encode, shard, parts=parts) for at, shard in order if at == stage]

    run(2)
    for hop in range(2, lines - 1):
        poll(hop)
    for i in range(lines - 1):
        for c in range(CHUNKS):
            take_line(i, c, None)
            take_other(i, c)
            if i == 2 and c < CHUNKS // 2:
                take_shared(CHUNKS // 2 + c)
            if i == lines - 2 and c == CHUNKS // 2:
                tasks += encodes(i, (0,))
            run(1 + c // 2 if i == 0 else -(-len(tasks) // (CHUNKS - c)))
        if i == 0 and lines > 2:
            for c in range(CHUNKS // 2, CHUNKS):
                extras_inner(c)
        tasks += encodes(i, (0, 1) if i < lines - 2 else (1,))
    tasks += encodes(lines, (0,))
    for c in range(CHUNKS - 1):
        take_other(lines - 1, c)
        if c == CHUNKS - 2:
            for gap in range(2, lines):
                take_far(gap, CHUNKS - 1)
        run(-(-len(tasks) // (CHUNKS - 1 - c)))
    for task in encodes(lines, (1,)):
        task()

    width = agg.shape[1] // 2
    my_first = pl.multiple_of(me * mesh_rows + core * half_mesh, half_mesh)

    def p_part(shard, q):
        flip, sub = q % 2, q // 2
        half = mate if flip else core
        first = shard * mesh_rows + half * half_mesh + sub * part_mesh
        return proj_all.at[pl.ds(pl.multiple_of(first, part_mesh), part_mesh)]

    for sub in range(SUBS):
        some = slice(sub * part_mesh, (sub + 1) * part_mesh)
        hidden = sum(
            jnp.dot(
                agg[some, h * width : (h + 1) * width].astype(jnp.bfloat16), w_node_all[h],
                preferred_element_type=jnp.float32,
            )
            for h in range(2)
        )
        projected = sum(
            jnp.dot(
                (
                    embed_all[h, some, :].astype(jnp.float32) + silu(hidden[:, h * width : (h + 1) * width])
                ).astype(jnp.bfloat16),
                w_dec_all[h], preferred_element_type=jnp.float32,
            )
            for h in range(2)
        ).astype(jnp.bfloat16)
        first_core = core == 0
        into = p_part(me, 2 * sub)
        proj_all[pl.ds(pl.multiple_of(my_first + sub * part_mesh, part_mesh), part_mesh), :] = jnp.where(
            first_core, projected[:, :cols], projected[:, cols:]
        )
        proj_mate[some, :] = jnp.where(first_core, projected[:, cols:], projected[:, :cols])
        for flip in range(2):
            ref = proj_mate.at[pl.ds(sub * part_mesh, part_mesh)] if flip else into
            chan = mate if flip else core
            routes = [(UP, has_up, up, pz_recv), (DOWN, has_down, down, pz_recv), (ACROSS, None, other, py_recv)]
            if lines > 2:
                routes[:0] = [
                    (UP, line == 0, (lines - 1) * 2 + side, pz_recv), (DOWN, line == lines - 1, side, pz_recv),
                ]
            for at, going, to, recv in routes:
                def go(ref=ref, into=into, at=at, to=to, recv=recv, q=2 * sub + flip, chan=chan):
                    remote(ref, into, p_send.at[at], recv.at[line, q], to, chan).start()
                if going is None:
                    go()
                else:
                    pl.when(going)(go)
    whole_half = proj_all.at[pl.ds(my_first, half_mesh)]
    remote(proj_mate, whole_half, p_send.at[MATE], pm_recv.at[0], me, mate).start()

    def decode(*shards):
        some = dec.at[0, pl.ds(0, half_grid)]
        for shard in shards:
            remote(some, some, dec_send.at[0], dec_recv.at[shard], me, mate).wait_recv()
        for t in range(2):
            at = pl.ds(t * half_grid, half_grid)
            acc[at, :] += sum(
                jnp.dot(
                    dec[shard, at, :], proj_all[pl.ds(pl.multiple_of(shard * mesh_rows, mesh_rows), mesh_rows), :],
                    preferred_element_type=jnp.float32,
                )
                for shard in shards
            )

    take_line, take_other, _, _, take_shared = relays(
        p_part, p_send, pz_recv, py_recv, lambda q: q >= EARLY, lambda shard, q: None, back=True)
    acc[...] = x_all[own_rows, pl.ds(pl.multiple_of(core * cols, cols), cols)].astype(jnp.float32)

    def own_decode():
        remote(proj_mate, whole_half, p_send.at[MATE], pm_recv.at[0], me, mate).wait_recv()
        decode(me)

    pieces = 2 * SUBS
    tasks += dec_tasks
    run(len(tasks))
    flush()
    tasks.append(own_decode)

    for q in range(pieces):
        take_line(0, q, "inner")
        if q:
            take_other(0, q - 1)
    take_other(0, pieces - 1)
    for q in range(pieces):
        take_shared(q)
    for q in range(pieces):
        take_line(0, q, "outer")
    for q in range(pieces):
        for i in range(1, lines - 1):
            take_line(i, q, "inner")
            take_line(i, q, "outer")
        if q % 2:
            run(1)
    run(len(tasks))
    early = [shard for at, shard in order_back if at < lines - 1]
    for n in range(0, len(early), 2):
        decode(*early[n : n + 2])
    for q in range(pieces):
        take_other(1, q)
    for at, shard in order_back:
        if at == lines - 1:
            decode(shard)
    for q in range(pieces):
        for i in range(2, lines):
            take_other(i, q)
    final = [shard for at, shard in order_back if at >= lines]
    if final:
        decode(*final)
    out_ref[...] = acc[...].astype(jnp.bfloat16)

    def drained(ref, sem):
        remote(ref, ref, sem, sem, me, mate).wait_send()

    for at in range(lines):
        @pl.when(line == at)
        def _(at=at):
            for n, (x_n, p_n) in enumerate(zip(link_pieces(at, lines, CHUNKS), return_pieces(at, lines, pieces))):
                if x_n:
                    drained(x_all.at[pl.ds(0, x_n * block)], x_send.at[n])
                    drained(proj_all.at[pl.ds(0, p_n * part_mesh)], p_send.at[n])
    drained(x_all.at[pl.ds(0, (peers - 1) * half_grid)], x_send.at[MATE])
    drained(proj_mate, p_send.at[MATE])
    drained(idx_own.at[pl.ds(0, peers - 1)], idx_send.at[0])
    drained(dec.at[:, pl.ds(0, half_grid)], dec_send.at[0])


def fused(grid_state, w_src, bias_src, mesh_embed, w_node, w_dec, slot_src, slot_dst, slot_count):
    peers = lax.axis_size("graph")
    capacity = slot_src.shape[2]
    grid_rows, chans = grid_state.shape
    mesh_rows = mesh_embed.shape[0]
    hidden = w_src.shape[1]
    lines = peers // 2
    bf16, f32, i32 = jnp.bfloat16, jnp.float32, jnp.int32
    dma = pltpu.SemaphoreType.DMA
    pieces = 2 * SUBS
    return pl.pallas_call(
        functools.partial(graph_kernel, peers),
        out_shape=jax.ShapeDtypeStruct((grid_rows, chans // 2), bf16),
        in_specs=[pl.BlockSpec(memory_space=pl.ANY)] * 9,
        out_specs=pl.BlockSpec(memory_space=pltpu.VMEM),
        scratch_shapes=[
            pltpu.VMEM((peers * grid_rows, chans), bf16),
            pltpu.VMEM((peers, 2, capacity), i32),
            pltpu.VMEM((peers, 2, capacity), i32),
            pltpu.VMEM(slot_src.shape, i32),
            pltpu.VMEM(slot_dst.shape, i32),
            pltpu.SMEM(slot_count.shape, i32),
            pltpu.VMEM((2,) + w_src.shape, bf16),
            pltpu.VMEM((2, 1, hidden), f32),
            pltpu.VMEM((2, mesh_rows // 2, hidden), bf16),
            pltpu.VMEM((2,) + w_node.shape, bf16),
            pltpu.VMEM((2,) + w_dec.shape, bf16),
            pltpu.VMEM((peers, mesh_rows // 2, grid_rows), bf16),
            pltpu.VMEM((peers, grid_rows, mesh_rows), bf16),
            pltpu.VMEM((mesh_rows, capacity), HOT),
            pltpu.VMEM((grid_rows, 2 * hidden), bf16),
            pltpu.VMEM((mesh_rows // 2, 2 * hidden), f32),
            pltpu.VMEM((grid_rows, chans // 2), f32),
            pltpu.VMEM((mesh_rows // 2, chans // 2), bf16),
            pltpu.VMEM((peers * mesh_rows, chans // 2), bf16),
            pltpu.SemaphoreType.REGULAR((2,)),
            dma((9,)), dma((5,)), dma((5,)), dma((1,)), dma((peers,)),
            dma((4,)), dma((lines, CHUNKS)), dma((lines, CHUNKS)), dma((peers, 2)),
            dma((4,)), dma((lines, pieces)), dma((lines, pieces)), dma((1,)), dma((1,)), dma((peers,)),
        ],
        compiler_params=pltpu.CompilerParams(collective_id=0, has_side_effects=True),
    )(grid_state, w_src, bias_src[None, :], mesh_embed, w_node, w_dec, slot_src, slot_dst, slot_count)


def held_bytes(peers, grid_state, mesh_embed, *rest):
    grid_rows, chans = grid_state.shape
    mesh_rows = mesh_embed.shape[0]
    return 2 * peers * grid_rows * (chans + 2 * mesh_rows)


def per_device(grid_state, w_src, bias_src, mesh_embed, *rest):
    peers = lax.axis_size("graph")
    fits = (
        peers % 2 == 0
        and peers in (4, 8)
        and lax.axis_size("chan") == 2
        and held_bytes(peers, grid_state, mesh_embed) <= VMEM_BUDGET
    )
    body = fused if fits else on_device
    return body(grid_state, w_src, bias_src, mesh_embed, *rest)


def solution(mesh):
    placed = (
        P(("member", "graph"), None),
        P(None, "chan"),
        P("chan"),
        P("graph", "chan"),
        P("chan", None),
        P("chan", None),
        P("graph", None, None),
        P(None, "graph", None),
        P(),
    )
    return jax.shard_map(
        per_device,
        mesh=mesh,
        in_specs=placed,
        out_specs=P(("member", "graph"), "chan"),
        check_vma=False,
    )
```

```python
import functools
import math

import jax
import jax.numpy as jnp
from jax import lax
from jax.experimental import pallas as pl
from jax.experimental.pallas import tpu as pltpu
from jax.sharding import PartitionSpec as P

CHUNKS = 4
SUBS = 2
EARLY = 1
HOT = jnp.float8_e4m3fn
VMEM_BUDGET = 48 * 2**20
MESH = pl.DeviceIdType.MESH
NT = (((1,), (1,)), ((), ()))


def edge_network(source_rows, w_src, bias_src):
    return jax.nn.silu(
        jnp.dot(source_rows, w_src, preferred_element_type=jnp.float32) + bias_src
    ).astype(jnp.bfloat16)


def segment_rows(values, indices, usable, row_count):
    slot_total = values.shape[0]
    width = values.shape[1]
    block_len = math.gcd(slot_total, 2048)
    block_count = slot_total // block_len
    targets = jnp.where(usable, indices, -1).reshape(block_count, block_len)
    pieces = values.reshape(block_count, block_len, width)
    row_ids = jnp.arange(row_count, dtype=jnp.int32)

    def add_block(summed, scan_item):
        row_target, piece_vals = scan_item
        one_hot = (row_ids[:, None] == row_target[None, :]).astype(jnp.bfloat16)
        return (summed + jnp.dot(one_hot, piece_vals, preferred_element_type=jnp.float32), None)

    result, unused = lax.scan(
        add_block, jnp.zeros((row_count, width), jnp.float32), (targets, pieces)
    )
    return result


def on_device(
    grid_state, w_src, bias_src, mesh_embed, w_node, w_dec, slot_src, slot_dst, slot_count
):
    peers = lax.axis_size("graph")
    own_index = lax.axis_index("graph")
    core_index = lax.axis_index("chan")
    capacity = slot_src.shape[2]
    positions = jnp.arange(capacity, dtype=jnp.int32)
    grid_rows = grid_state.shape[0]
    mesh_rows = mesh_embed.shape[0]
    sent_counts = lax.dynamic_slice_in_dim(slot_count, own_index, 1, 0)[0]
    recv_counts = lax.dynamic_slice_in_dim(slot_count, own_index, 1, 1)[:, 0]
    half_slots = capacity // 2
    chosen = lax.dynamic_slice_in_dim(slot_src[0], core_index * half_slots, half_slots, 1)
    picked = jnp.take(grid_state, chosen.reshape(-1), axis=0).reshape(
        peers, half_slots, grid_state.shape[1]
    )
    arrived = lax.all_to_all(picked, "graph", split_axis=0, concat_axis=0, tiled=True)
    joined = lax.all_gather(arrived, "chan", axis=1, tiled=True)
    messages = edge_network(joined.reshape(peers * capacity, grid_state.shape[1]), w_src, bias_src)
    arrive_ok = (positions[None, :] < recv_counts[:, None]).reshape(-1)
    dst_rows = slot_dst[:, 0, :].reshape(-1)
    aggregate = segment_rows(messages, dst_rows, arrive_ok, mesh_rows)
    partial_hidden = jnp.dot(
        aggregate.astype(jnp.bfloat16), w_node, preferred_element_type=jnp.float32
    )
    hidden_pre = lax.psum_scatter(partial_hidden, "chan", scatter_dimension=1, tiled=True)
    latent = (mesh_embed.astype(jnp.float32) + jax.nn.silu(hidden_pre)).astype(jnp.bfloat16)
    partial_proj = jnp.dot(latent, w_dec, preferred_element_type=jnp.float32)
    projected = lax.psum_scatter(partial_proj, "chan", scatter_dimension=1, tiled=True).astype(
        jnp.bfloat16
    )
    returned = jnp.take(projected, dst_rows, axis=0).reshape(peers, capacity, projected.shape[1])
    came_back = lax.all_to_all(returned, "graph", split_axis=0, concat_axis=0, tiled=True).reshape(
        peers * capacity, projected.shape[1]
    )
    send_ok = (positions[None, :] < sent_counts[:, None]).reshape(-1)
    decoded = segment_rows(came_back, slot_src[0].reshape(-1), send_ok, grid_rows)
    width_half = decoded.shape[1]
    own_cols = lax.dynamic_slice_in_dim(grid_state, core_index * width_half, width_half, 1)
    return (own_cols.astype(jnp.float32) + decoded).astype(jnp.bfloat16)


def silu(v):
    half = 0.5 * v
    return half + half * jnp.tanh(half)


def one_hot(first, rows, indices):
    row_ids = lax.broadcasted_iota(jnp.int16, (rows, indices.shape[1]), 0)
    hits = row_ids == (indices - first).astype(jnp.int16)
    return jnp.where(hits, jnp.bfloat16(1), jnp.bfloat16(0)).astype(HOT)


def is_end(line, lines):
    return line in (0, lines - 1)


def given(line, lines):
    outer = line - 1 if line < lines // 2 else line + 1
    return outer if not is_end(line, lines) and is_end(outer, lines) else None


def arrival_order(line, lines):
    stages = [(0, 1, 0, line)]
    for source in range(lines):
        gap = abs(source - line)
        if gap:
            split = is_end(line, lines) and gap > 1
            shared = given(line, lines) is not None and gap == 1 and source != given(line, lines)
            stages += [(gap - 1, 0, gap, source), (lines if split else 2 if shared else gap, 1, gap, source)]
    return sorted(stages)


def link_pieces(line, lines, pieces):
    def extra(to):
        if not 0 <= to < lines:
            return 0
        if is_end(to, lines):
            return lines - 2
        return 0 if given(to, lines) is None else pieces if given(to, lines) == line else pieces // 2

    up = pieces * (line + 1) + extra(line + 1) if line < lines - 1 else 0
    down = pieces * (lines - line) + extra(line - 1) if line > 0 else 0
    across = pieces * lines
    if given(line, lines) is not None:
        across -= pieces + pieces // 2
    if is_end(line, lines):
        across -= lines - 2
    return up, down, across


def return_order(line, lines):
    stages = [(0, 1, 0, line)]
    for source in range(lines):
        gap = abs(source - line)
        if gap:
            stages += [(gap - 1, 0, gap, source), (lines - 2 + gap, 1, gap, source)]
    return sorted(stages)


def return_pieces(line, lines, pieces):
    direct = lines > 2

    def one_way(to, behind, first):
        if not 0 <= to < lines:
            return 0
        onward = behind - (1 if direct and is_end(to, lines) and behind else 0)
        beside = pieces - EARLY if direct and is_end(to, lines) else pieces if given(to, lines) == line else 0
        return pieces * (1 + (1 if direct and first else 0) + onward) + beside

    up = one_way(line + 1, line, line == 0)
    down = one_way(line - 1, lines - 1 - line, line == lines - 1)
    skipped = pieces if given(line, lines) is not None else pieces - EARLY if lines > 2 and is_end(line, lines) else 0
    return up, down, pieces * lines - skipped


class Shifted:
    def __init__(self, ref, first):
        self.ref, self.first, self.at = ref, first, self

    def __getitem__(self, index):
        return self.ref.at[self.first + index]


def graph_kernel(
    peers,
    x_ref, w_src_ref, bias_ref, embed_ref, w_node_ref, w_dec_ref, src_ref, dst_ref, count_ref,
    out_ref,
    x_all, idx_own, idx_in, src_vmem, dst_vmem, count_smem, w_src_all, bias_all, embed_all, w_node_all, w_dec_all,
    enc, dec, hot, msg, agg, acc, out_vmem, proj_mate, proj_all,
    ready, local_sem, par_recv, idx_send, idx_recv,
    x_send, xz_recv, xy_recv, xm_recv, pz_recv, py_recv, pm_recv, dec_send, dec_recv,
):
    par_send = p_send = Shifted(local_sem, 4)
    lines = peers // 2
    me = lax.axis_index("graph")
    core = lax.axis_index("chan")
    mate = 1 - core
    line, side = me // 2, me % 2
    other = line * 2 + (1 - side)
    up, down = (line + 1) * 2 + side, (line - 1) * 2 + side
    has_up, has_down = line < lines - 1, line > 0
    low_half = line < lines // 2
    grid_rows, chans = x_ref.shape
    half_grid = grid_rows // 2
    block = half_grid // CHUNKS
    mesh_rows = embed_ref.shape[0]
    half_mesh = mesh_rows // 2
    part_mesh = half_mesh // SUBS
    cols = chans // 2
    capacity = src_ref.shape[2]
    UP, DOWN, ACROSS, MATE = range(4)

    def remote(src, dst, send, recv, graph, chan):
        return pltpu.make_async_remote_copy(
            src_ref=src, dst_ref=dst, send_sem=send, recv_sem=recv,
            device_id={"graph": graph, "chan": chan}, device_id_type=MESH,
        )

    def by_line(values):
        return sum(jnp.where(line == at, values[at], 0) for at in range(lines))

    end = (line == 0) | (line == lines - 1)
    giver = by_line([-1 if given(at, lines) is None else given(at, lines) for at in range(lines)])
    barrier = pltpu.get_barrier_semaphore()

    def greet(graph, chan):
        pl.semaphore_signal(barrier, inc=1, device_id={"graph": graph, "chan": chan}, device_id_type=MESH)

    greet(me, mate)
    for chan in (core, mate):
        greet(other, chan)
        pl.when(has_up)(functools.partial(greet, up, chan))
        pl.when(has_down)(functools.partial(greet, down, chan))
    my_rows = pl.ds(pl.multiple_of(core * half_mesh, half_mesh), half_mesh)
    mate_rows = pl.ds(pl.multiple_of(mate * half_mesh, half_mesh), half_mesh)
    own_rows = pl.ds(pl.multiple_of(me * grid_rows, grid_rows), grid_rows)
    locals_ = [
        pltpu.make_async_copy(src_ref, src_vmem, local_sem.at[0]),
        pltpu.make_async_copy(dst_ref, dst_vmem, local_sem.at[1]),
        pltpu.make_async_copy(count_ref, count_smem, local_sem.at[2]),
        pltpu.make_async_copy(x_ref, x_all.at[own_rows], local_sem.at[3]),
        pltpu.make_async_copy(w_src_ref, w_src_all.at[core], local_sem.at[4]),
        pltpu.make_async_copy(bias_ref, bias_all.at[core], local_sem.at[5]),
        pltpu.make_async_copy(w_node_ref, w_node_all.at[core], local_sem.at[6]),
        pltpu.make_async_copy(w_dec_ref, w_dec_all.at[core], local_sem.at[7]),
        pltpu.make_async_copy(embed_ref.at[my_rows], embed_all.at[core], local_sem.at[8]),
    ]
    for copy in locals_[3:4] + locals_[:3] + locals_[4:]:
        copy.start()
    locals_[3].wait()
    pl.semaphore_wait(barrier, 3 + 2 * jnp.where(has_up, 1, 0) + 2 * jnp.where(has_down, 1, 0))

    def x_part(shard, c, half=core):
        first = shard * grid_rows + c * 2 * block + half * block
        return x_all.at[pl.ds(pl.multiple_of(first, block), block)]

    def send_own(c):
        ref = x_part(me, c)
        for at, going, to, recv in (
            (UP, has_up, up, xz_recv), (DOWN, has_down, down, xz_recv), (ACROSS, None, other, xy_recv),
        ):
            def go(at=at, to=to, recv=recv):
                remote(ref, ref, x_send.at[at], recv.at[line, c], to, core).start()
            if going is None:
                go()
            else:
                pl.when(going)(go)

    send_own(0)
    for copy in locals_[:3]:
        copy.wait()
    slots = lax.broadcasted_iota(jnp.int32, (1, capacity), 1)
    for to in range(peers):
        idx_own[to, 0:1, :] = jnp.where(slots < count_smem[me, to], src_vmem[0, to : to + 1, :], -1)
        idx_own[to, 1:2, :] = dst_vmem[to]
    idx_in[me] = idx_own[me]

    def send_idx(to):
        remote(idx_own.at[to], idx_in.at[me], idx_send.at[0], idx_recv.at[me], to, core).start()

    send_idx(other)
    pl.when(has_up)(functools.partial(send_idx, up))
    pl.when(has_down)(functools.partial(send_idx, down))
    for c in range(1, CHUNKS - 1):
        send_own(c)
    for copy in locals_[4:]:
        copy.wait()
    par_copies = [
        remote(w_src_all.at[core], w_src_all.at[core], par_send.at[0], par_recv.at[0], me, mate),
        remote(bias_all.at[core], bias_all.at[core], par_send.at[1], par_recv.at[1], me, mate),
        remote(embed_ref.at[mate_rows], embed_all.at[core], par_send.at[2], par_recv.at[2], me, mate),
        remote(w_node_all.at[core], w_node_all.at[core], par_send.at[3], par_recv.at[3], me, mate),
        remote(w_dec_all.at[core], w_dec_all.at[core], par_send.at[4], par_recv.at[4], me, mate),
    ]
    for copy in par_copies:
        copy.start()

    def tell(at, to):
        pl.semaphore_signal(ready.at[at], inc=1, device_id={"graph": to, "chan": core}, device_id_type=MESH)

    pl.when(line == 0)(functools.partial(tell, 0, up))
    pl.when(line == lines - 1)(functools.partial(tell, 1, down))

    def relays(part, send, z_recv, y_recv, late, arrived, back=False):
        def extra(source, q, above):
            ref = part(source * 2 + 1 - side, q)
            remote(ref, ref, send.at[UP if above else DOWN], y_recv.at[source, q], up if above else down, core).start()

        def extras(source, q):
            for above, there in ((True, has_up), (False, has_down)):
                to = line + 1 if above else line - 1
                to_end = (to == 0) | (to == lines - 1)
                to_giver = by_line([
                    -1 if not 0 <= at + (1 if above else -1) < lines
                    or given(at + (1 if above else -1), lines) is None
                    else given(at + (1 if above else -1), lines)
                    for at in range(lines)
                ])
                wanted = (source == line) & (to_giver == line)
                if late(q):
                    gap_to = jnp.abs(source - to)
                    wanted = wanted | (to_end & ((gap_to == 2) if back else (gap_to > 1)))
                pl.when(there & wanted)(functools.partial(extra, source, q, above))

        def extras_inner(q):
            for above, there in ((True, has_up), (False, has_down)):
                step = 1 if above else -1
                wanted = by_line([
                    1 if 0 <= at + step < lines and given(at + step, lines) not in (None, at) else 0 for at in range(lines)
                ]) == 1
                pl.when(there & wanted)(functools.partial(extra, line, q, above))

        def take_line(i, q, which):
            for above in (True, False):
                source = line + 1 + i if above else line - 1 - i
                valid = (source < lines) if above else (source >= 0)
                if which is not None:
                    valid = valid & ((low_half if above else jnp.logical_not(low_half)) == (which == "inner"))
                onward, to, at = (has_down, down, DOWN) if above else (has_up, up, UP)

                @pl.when(valid)
                def _(source=source, onward=onward, to=to, at=at):
                    ref = part(source * 2 + side, q)
                    remote(ref, ref, send.at[at], z_recv.at[source, q], me, mate).wait_recv()

                    if back and lines > 2:
                        to_line = line - 1 if above else line + 1
                        onward = onward & ((to_line != (0 if above else lines - 1)) | (source != (lines - 1 if above else 0)))

                    @pl.when(onward)
                    def _():
                        remote(ref, ref, send.at[at], z_recv.at[source, q], to, core).start()

                    crossing = source != giver
                    if not back and q >= CHUNKS // 2:
                        crossing = crossing & ((giver < 0) | (jnp.abs(source - line) != 1))
                    if late(q):
                        gap_of = jnp.abs(source - line)
                        crossing = crossing & jnp.logical_not(end & ((gap_of == 2) if back else (gap_of > 1)))

                    @pl.when(crossing)
                    def _():
                        remote(ref, ref, send.at[ACROSS], y_recv.at[source, q], other, core).start()

                    arrived(source * 2 + side, q)

        def take_other(i, q):
            def take(source):
                shard = source * 2 + 1 - side
                ref = part(shard, q)
                remote(ref, ref, send.at[ACROSS], y_recv.at[source, q], me, mate).wait_recv()
                extras(source, q)
                arrived(shard, q)

            if i == 0:
                take(line)
                return
            for source, valid in ((line + i, line + i < lines), (line - i, line - i >= 0)):
                if late(q) and not back and i > 1:
                    valid = valid & jnp.logical_not(end)
                if i == 1 and (back or q >= CHUNKS // 2):
                    valid = valid & ((giver < 0) | (source == giver))
                pl.when(valid)(functools.partial(take, source))

        def take_far(i, q):
            pl.when(end)(functools.partial(take_one, jnp.where(low_half, line + i, line - i), q))

        def take_one(source, q, onward=False):
            shard = source * 2 + 1 - side
            ref = part(shard, q)
            remote(ref, ref, send.at[ACROSS], y_recv.at[source, q], me, mate).wait_recv()
            if onward:
                extras(source, q)
            arrived(shard, q)

        def take_shared(q):
            source = jnp.where(low_half, line + 1, line - 1)
            pl.when(giver >= 0)(functools.partial(take_one, source, q, onward=True))

        return take_line, take_other, take_far, extras_inner, take_shared

    def to_mate(shard, c):
        ref = x_part(shard, c)
        remote(ref, ref, x_send.at[MATE], xm_recv.at[shard, c // (CHUNKS // 2)], me, mate).start()

    nearest = [sorted((p for p in range(lines) if p != at), key=lambda p: (abs(p - at), p)) for at in range(lines)]
    sources = [by_line([nearest[at][i] for at in range(lines)]) for i in range(lines - 1)]
    build_order = [me, other]
    for i in range(lines):
        build_order += [source * 2 + side for source in sources[i : i + 1]]
        build_order += [source * 2 + 1 - side for source in sources[max(i - 1, 0) : i]]

    def by_stage(rule):
        tables = [rule(at, lines) for at in range(lines)]
        found = []
        for k in range(peers - 1):
            source = by_line([tables[at][k][3] for at in range(lines)])
            flip = by_line([tables[at][k][1] for at in range(lines)])
            stage = max(tables[at][k][0] for at in range(lines))
            found.append((stage, source * 2 + jnp.where(flip == 1, 1 - side, side)))
        return found

    order, order_back = by_stage(arrival_order), by_stage(return_order)

    def build_enc(shard, wait=True):
        if wait:
            remote(idx_own.at[0], idx_in.at[shard], idx_send.at[0], idx_recv.at[shard], me, mate).wait_recv()
        hot[:half_mesh, :] = one_hot(core * half_mesh, half_mesh, dst_vmem[shard])
        for t in range(2):
            picks = one_hot(t * half_grid, half_grid, idx_in[shard, 0:1, :])
            enc[shard, :, t * half_grid : (t + 1) * half_grid] = lax.dot_general(
                hot[:half_mesh, :], picks, NT, preferred_element_type=jnp.float32
            ).astype(jnp.bfloat16)

    pending = []

    def dec_copy(shard, half):
        ref = dec.at[shard, pl.ds(pl.multiple_of(half * half_grid, half_grid), half_grid)]
        return remote(ref, ref, dec_send.at[0], dec_recv.at[shard], me, mate)

    def flush():
        while pending:
            dec_copy(pending.pop(0), core).start()

    def build_dec(shard, wait=True):
        flush()
        hot[...] = one_hot(0, mesh_rows, idx_in[shard, 1:2, :])
        for t in range(half_grid // 256):
            first = pl.multiple_of(core * half_grid, half_grid) + t * 256
            picks = one_hot(first, 256, idx_own[shard, 0:1, :])
            dec[shard, pl.ds(pl.multiple_of(first, 256), 256), :] = lax.dot_general(
                picks, hot[...], NT, preferred_element_type=jnp.float32
            ).astype(jnp.bfloat16)
        pending.append(shard)

    def encode(shard, first=False, parts=(0, 1)):
        if not first:
            for part in parts:
                some = x_all.at[pl.ds(0, half_grid // 2)]
                remote(some, some, x_send.at[MATE], xm_recv.at[shard, part], me, mate).wait_recv()
        low, high = min(parts) * CHUNKS // 2, (max(parts) + 1) * CHUNKS // 2
        for c in range(low, high):
            rows = pl.ds(pl.multiple_of(shard * grid_rows, grid_rows) + c * 2 * block, 2 * block)
            for h in range(2):
                pre = jnp.dot(x_all[rows, :], w_src_all[h], preferred_element_type=jnp.float32) + bias_all[h]
                msg[c * 2 * block : (c + 1) * 2 * block, h * (msg.shape[1] // 2) : (h + 1) * (msg.shape[1] // 2)] = (
                    pre + pre * jnp.tanh(pre)
                ).astype(jnp.bfloat16)
        some = slice(low * 2 * block, high * 2 * block)
        total = jnp.dot(enc[shard, :, some], msg[some, :], preferred_element_type=jnp.float32)
        if first:
            agg[...] = total
        else:
            agg[...] += total

    def poll(hop):
        @pl.when(line == hop + 1)
        def _():
            pl.semaphore_wait(ready.at[0], 1)
            pl.when(has_up)(functools.partial(tell, 0, up))

        @pl.when(line == lines - 2 - hop)
        def _():
            pl.semaphore_wait(ready.at[1], 1)
            pl.when(has_down)(functools.partial(tell, 1, down))

        known = by_line([max(at - 1, lines - 2 - at) for at in range(lines)]) == hop
        for source in range(lines):
            for its_side in range(2):
                near = jnp.where(side == its_side, jnp.abs(line - source), 2 * jnp.abs(line - source) + 1) <= 1
                pl.when(known & jnp.logical_not(near))(functools.partial(send_idx, source * 2 + its_side))

    poll(0)
    build_enc(me, wait=False)
    build_dec(me, wait=False)
    for copy in par_copies:
        copy.wait()
    w_src_all[...] = w_src_all[...] * 0.5
    bias_all[...] = bias_all[...] * 0.5
    encode(me, first=True)
    poll(1)
    send_own(CHUNKS - 1)
    enc_tasks = [functools.partial(build_enc, shard) for shard in build_order[1:]]
    dec_tasks = [functools.partial(build_dec, shard, wait=False) for shard in build_order[1:]]
    tasks = [task for pair in zip(enc_tasks[:-2], dec_tasks[:-2]) for task in pair] + enc_tasks[-2:]
    dec_tasks = dec_tasks[-2:]

    def run(count):
        for _ in range(min(count, len(tasks))):
            tasks.pop(0)()

    def halves(c):
        return c == CHUNKS - 1

    take_line, take_other, take_far, extras_inner, take_shared = relays(x_part, x_send, xz_recv, xy_recv, halves, to_mate)
    def encodes(stage, parts):
        return [functools.partial(encode, shard, parts=parts) for at, shard in order if at == stage]

    run(2)
    for hop in range(2, lines - 1):
        poll(hop)
    for i in range(lines - 1):
        for c in range(CHUNKS):
            take_line(i, c, None)
            take_other(i, c)
            if i == 2 and c < CHUNKS // 2:
                take_shared(CHUNKS // 2 + c)
            if i == lines - 2 and c == CHUNKS // 2:
                tasks += encodes(i, (0,))
            run(1 + c // 2 if i == 0 else -(-len(tasks) // (CHUNKS - c)))
        if i == 0 and lines > 2:
            for c in range(CHUNKS // 2, CHUNKS):
                extras_inner(c)
        tasks += encodes(i, (0, 1) if i < lines - 2 else (1,))
    tasks += encodes(lines, (0,))
    for c in range(CHUNKS - 1):
        take_other(lines - 1, c)
        if c == CHUNKS - 2:
            for gap in range(2, lines):
                take_far(gap, CHUNKS - 1)
        run(-(-len(tasks) // (CHUNKS - 1 - c)))
    for task in encodes(lines, (1,)):
        task()

    width = agg.shape[1] // 2
    my_first = pl.multiple_of(me * mesh_rows + core * half_mesh, half_mesh)

    def p_part(shard, q):
        flip, sub = q % 2, q // 2
        half = mate if flip else core
        first = shard * mesh_rows + half * half_mesh + sub * part_mesh
        return proj_all.at[pl.ds(pl.multiple_of(first, part_mesh), part_mesh)]

    for sub in range(SUBS):
        some = slice(sub * part_mesh, (sub + 1) * part_mesh)
        hidden = sum(
            jnp.dot(
                agg[some, h * width : (h + 1) * width].astype(jnp.bfloat16), w_node_all[h],
                preferred_element_type=jnp.float32,
            )
            for h in range(2)
        )
        projected = sum(
            jnp.dot(
                (
                    embed_all[h, some, :].astype(jnp.float32) + silu(hidden[:, h * width : (h + 1) * width])
                ).astype(jnp.bfloat16),
                w_dec_all[h], preferred_element_type=jnp.float32,
            )
            for h in range(2)
        ).astype(jnp.bfloat16)
        first_core = core == 0
        into = p_part(me, 2 * sub)
        proj_all[pl.ds(pl.multiple_of(my_first + sub * part_mesh, part_mesh), part_mesh), :] = jnp.where(
            first_core, projected[:, :cols], projected[:, cols:]
        )
        proj_mate[some, :] = jnp.where(first_core, projected[:, cols:], projected[:, :cols])
        for flip in range(2):
            ref = proj_mate.at[pl.ds(sub * part_mesh, part_mesh)] if flip else into
            chan = mate if flip else core
            routes = [(UP, has_up, up, pz_recv), (DOWN, has_down, down, pz_recv), (ACROSS, None, other, py_recv)]
            if lines > 2:
                routes[:0] = [
                    (UP, line == 0, (lines - 1) * 2 + side, pz_recv), (DOWN, line == lines - 1, side, pz_recv),
                ]
            for at, going, to, recv in routes:
                def go(ref=ref, into=into, at=at, to=to, recv=recv, q=2 * sub + flip, chan=chan):
                    remote(ref, into, p_send.at[at], recv.at[line, q], to, chan).start()
                if going is None:
                    go()
                else:
                    pl.when(going)(go)
    whole_half = proj_all.at[pl.ds(my_first, half_mesh)]
    remote(proj_mate, whole_half, p_send.at[MATE], pm_recv.at[0], me, mate).start()

    def arrived_dec(*shards):
        some = dec.at[0, pl.ds(0, half_grid)]
        for shard in shards:
            remote(some, some, dec_send.at[0], dec_recv.at[shard], me, mate).wait_recv()

    def products(at, shards):
        return sum(
            jnp.dot(
                dec[shard, at, :], proj_all[pl.ds(pl.multiple_of(shard * mesh_rows, mesh_rows), mesh_rows), :],
                preferred_element_type=jnp.float32,
            )
            for shard in shards
        )

    def decode(*shards):
        arrived_dec(*shards)
        for t in range(2):
            at = pl.ds(t * half_grid, half_grid)
            acc[at, :] += products(at, shards)

    take_line, take_other, _, _, take_shared = relays(
        p_part, p_send, pz_recv, py_recv, lambda q: q >= EARLY, lambda shard, q: None, back=True)
    acc[...] = x_all[own_rows, pl.ds(pl.multiple_of(core * cols, cols), cols)].astype(jnp.float32)

    def own_decode():
        remote(proj_mate, whole_half, p_send.at[MATE], pm_recv.at[0], me, mate).wait_recv()
        decode(me)

    pieces = 2 * SUBS
    tasks += dec_tasks
    run(len(tasks))
    flush()
    tasks.append(own_decode)

    for q in range(pieces):
        take_line(0, q, "inner")
        if q:
            take_other(0, q - 1)
    take_other(0, pieces - 1)
    for q in range(pieces):
        take_shared(q)
    for q in range(pieces):
        take_line(0, q, "outer")
    for q in range(pieces):
        for i in range(1, lines - 1):
            take_line(i, q, "inner")
            take_line(i, q, "outer")
        if q % 2:
            run(1)
    run(len(tasks))
    early = [shard for at, shard in order_back if at < lines - 1]
    for n in range(0, len(early), 2):
        decode(*early[n : n + 2])
    for q in range(pieces):
        take_other(1, q)
    for at, shard in order_back:
        if at == lines - 1:
            decode(shard)
    for q in range(pieces):
        for i in range(2, lines):
            take_other(i, q)
    final = [shard for at, shard in order_back if at >= lines]
    arrived_dec(*final)
    outs = []
    for t in range(2):
        at = pl.ds(t * half_grid, half_grid)
        out_vmem[at, :] = (acc[at, :] + products(at, final)).astype(jnp.bfloat16)
        outs.append(pltpu.make_async_copy(out_vmem.at[at], out_ref.at[at], local_sem.at[t]))
        outs[t].start()

    def drained(ref, sem):
        remote(ref, ref, sem, sem, me, mate).wait_send()

    for at in range(lines):
        @pl.when(line == at)
        def _(at=at):
            for n, (x_n, p_n) in enumerate(zip(link_pieces(at, lines, CHUNKS), return_pieces(at, lines, pieces))):
                if x_n:
                    drained(x_all.at[pl.ds(0, x_n * block)], x_send.at[n])
                    drained(proj_all.at[pl.ds(0, p_n * part_mesh)], p_send.at[n])
    drained(x_all.at[pl.ds(0, (peers - 1) * half_grid)], x_send.at[MATE])
    drained(proj_mate, p_send.at[MATE])
    drained(idx_own.at[pl.ds(0, peers - 1)], idx_send.at[0])
    drained(dec.at[:, pl.ds(0, half_grid)], dec_send.at[0])
    for copy in outs:
        copy.wait()


def fused(grid_state, w_src, bias_src, mesh_embed, w_node, w_dec, slot_src, slot_dst, slot_count):
    peers = lax.axis_size("graph")
    capacity = slot_src.shape[2]
    grid_rows, chans = grid_state.shape
    mesh_rows = mesh_embed.shape[0]
    hidden = w_src.shape[1]
    lines = peers // 2
    bf16, f32, i32 = jnp.bfloat16, jnp.float32, jnp.int32
    dma = pltpu.SemaphoreType.DMA
    pieces = 2 * SUBS
    return pl.pallas_call(
        functools.partial(graph_kernel, peers),
        out_shape=jax.ShapeDtypeStruct((grid_rows, chans // 2), bf16),
        in_specs=[pl.BlockSpec(memory_space=pl.ANY)] * 9,
        out_specs=pl.BlockSpec(memory_space=pl.ANY),
        scratch_shapes=[
            pltpu.VMEM((peers * grid_rows, chans), bf16),
            pltpu.VMEM((peers, 2, capacity), i32),
            pltpu.VMEM((peers, 2, capacity), i32),
            pltpu.VMEM(slot_src.shape, i32),
            pltpu.VMEM(slot_dst.shape, i32),
            pltpu.SMEM(slot_count.shape, i32),
            pltpu.VMEM((2,) + w_src.shape, bf16),
            pltpu.VMEM((2, 1, hidden), f32),
            pltpu.VMEM((2, mesh_rows // 2, hidden), bf16),
            pltpu.VMEM((2,) + w_node.shape, bf16),
            pltpu.VMEM((2,) + w_dec.shape, bf16),
            pltpu.VMEM((peers, mesh_rows // 2, grid_rows), bf16),
            pltpu.VMEM((peers, grid_rows, mesh_rows), bf16),
            pltpu.VMEM((mesh_rows, capacity), HOT),
            pltpu.VMEM((grid_rows, 2 * hidden), bf16),
            pltpu.VMEM((mesh_rows // 2, 2 * hidden), f32),
            pltpu.VMEM((grid_rows, chans // 2), f32),
            pltpu.VMEM((grid_rows, chans // 2), bf16),
            pltpu.VMEM((mesh_rows // 2, chans // 2), bf16),
            pltpu.VMEM((peers * mesh_rows, chans // 2), bf16),
            pltpu.SemaphoreType.REGULAR((2,)),
            dma((9,)), dma((5,)), dma((1,)), dma((peers,)),
            dma((4,)), dma((lines, CHUNKS)), dma((lines, CHUNKS)), dma((peers, 2)),
            dma((lines, pieces)), dma((lines, pieces)), dma((1,)), dma((1,)), dma((peers,)),
        ],
        compiler_params=pltpu.CompilerParams(collective_id=0, has_side_effects=True),
    )(grid_state, w_src, bias_src[None, :], mesh_embed, w_node, w_dec, slot_src, slot_dst, slot_count)


def held_bytes(peers, grid_state, mesh_embed, *rest):
    grid_rows, chans = grid_state.shape
    mesh_rows = mesh_embed.shape[0]
    return 2 * peers * grid_rows * (chans + 2 * mesh_rows)


def per_device(grid_state, w_src, bias_src, mesh_embed, *rest):
    peers = lax.axis_size("graph")
    fits = (
        peers == 2 * CHUNKS
        and lax.axis_size("chan") == 2
        and held_bytes(peers, grid_state, mesh_embed) <= VMEM_BUDGET
    )
    body = fused if fits else on_device
    return body(grid_state, w_src, bias_src, mesh_embed, *rest)


def solution(mesh):
    placed = (
        P(("member", "graph"), None),
        P(None, "chan"),
        P("chan"),
        P("graph", "chan"),
        P("chan", None),
        P("chan", None),
        P("graph", None, None),
        P(None, "graph", None),
        P(),
    )
    return jax.shard_map(
        per_device,
        mesh=mesh,
        in_specs=placed,
        out_specs=P(("member", "graph"), "chan"),
        check_vma=False,
    )
```
